768 devices in a mesh: clip: 192 (over y, z, core), seq: 4 (over x).
Axes of the slice: x: 4, y: 8, z: 12, core: 2. Of those that a mesh axis runs over, the one named last changes fastest.
Arguments:
- patches: bfloat16 [49152, 1280], P('clip'), may hold values from -6 to 6
- clip_tokens: int32 [192], P('clip'), may hold values from 16 to 64
- positions: int32 [192, 64], P('clip'), may hold values from 0 to 255, as said below
- norm_gain: float32 [1280], replicated, may hold values from 0.5 to 1.5
- norm_bias: float32 [1280], replicated, may hold values from -3 to 3
- w_qkv: bfloat16 [1280, 3, 1280], P(None, None, 'seq'), may hold values from -0.9503289 to 0.9503289
- b_qkv: float32 [3, 1280], P(None, 'seq'), may hold values from -3 to 3
- w_proj: bfloat16 [1280, 1280], P('seq'), may hold values from -0.15625 to 0.15625
- b_proj: float32 [1280], replicated, may hold values from -3 to 3
- merge_gain: float32 [1280], replicated, may hold values from 0.5 to 1.5
- merge_bias: float32 [1280], replicated, may hold values from -3 to 3
- grad_placed: bfloat16 [49152, 5120], P(('clip', 'seq')), may hold values from -0.026977539 to 0.026977539
Outputs:
- placed: bfloat16 [49152, 5120], P(('clip', 'seq'))
- grad_qkv: float32 [4, 960, 1280], P('seq', 'clip')
The draws below stay inside these ranges and needn't reach their ends.
Inputs may be any that keep to these rules, and one draw needn't show every extreme that they name: The positions of one clip are distinct.
All inputs are finite; a program needn't handle non-finite values.
Results may differ from the reference program's by a relative error of at most 0.01.
Values may be sent and summed in bfloat16 or wider, within the bound.
A program may use at most 64 MiB of HBM per device.

```python
import jax
import jax.numpy as jnp
from jax import lax

D = 1280
HEADS = 16
BLOCK = 256
HEAD = 80
TOKENS_CLIP = 64
LEN = 256
GROUPS = 192
N_SEQ = 4


def draw_positions(key, part):
    subkeys = jax.random.split(key, GROUPS)
    rows = jax.vmap(lambda single: jax.random.permutation(single, LEN)[:TOKENS_CLIP])(subkeys)
    return rows.astype(jnp.int32)


def draw_w_qkv(key, part):
    spread = D ** (-0.5)
    base = jnp.clip(jax.random.normal(key, (D, 3, D), jnp.float32), -6.0, 6.0) * spread
    return base.astype(jnp.bfloat16)


def plant(result, stream_key, least, top_value):
    dims = result.shape
    place = [jax.random.randint(jax.random.fold_in(stream_key, axis), (), 0, dims[axis]) for axis in range(len(dims))]
    result = result.at[tuple(place)].set(least)
    longest = dims.index(max(dims))
    place[longest] = (place[longest] + 1) % dims[longest]
    return result.at[tuple(place)].set(top_value)


def steps_of(own_key, dims, shards, least, largest):
    def one(dim, shards_of):
        heights = jax.random.uniform(jax.random.fold_in(jax.random.fold_in(own_key, 6), dim), (shards_of,), jnp.float32, least / len(shards), largest / len(shards))
        return jnp.repeat(jnp.exp(heights), dims[dim] // shards_of).reshape((-1,) + (1,) * (len(dims) - dim - 1))

    factor_of = one(*shards[0])
    for cut in shards[1:]:
        factor_of = factor_of * one(*cut)
    return factor_of


def gaussian(key, shape, width, bound, cuts=(), held_as=jnp.bfloat16):
    values = jax.random.normal(key, shape, jnp.float32) * width
    if len(cuts) > 0:
        values = steps_of(key, shape, cuts, -0.22, 0.18) * values
    return jnp.clip(values, min=-bound, max=bound).astype(held_as)


def setup_inputs(seed: int = 0) -> dict:
    streams_of = jax.random.split(jax.random.key(seed), 13)
    patches = gaussian(streams_of[0], (GROUPS * BLOCK, D), 1.0, 6.0, ((0, 192),))
    clip_tokens = plant(jax.random.randint(streams_of[1], (GROUPS,), BLOCK // 16, BLOCK // 4 + 1), jax.random.fold_in(streams_of[1], 1), BLOCK // 16, (BLOCK // 4 + 1) - 1).astype(jnp.int32)
    positions = draw_positions(jax.random.fold_in(streams_of[12], 71), 0)
    norm_gain = jnp.clip(1.0 + 0.1 * jax.random.normal(streams_of[3], (D,), jnp.float32), 0.5, 1.5)
    norm_bias = gaussian(streams_of[4], (D,), 0.5, 3.0, (), jnp.float32)
    w_qkv = draw_w_qkv(jax.random.fold_in(streams_of[12], 71), 0)
    b_qkv = gaussian(streams_of[6], (3, D), 0.5, 3.0, ((1, 4),), jnp.float32)
    w_proj = gaussian(streams_of[7], (D, D), D ** -0.5, 0.15625, ((0, 4),))
    b_proj = gaussian(streams_of[8], (D,), 0.5, 3.0, (), jnp.float32)
    merge_gain = jnp.clip(1.0 + 0.1 * jax.random.normal(streams_of[9], (D,), jnp.float32), 0.5, 1.5)
    merge_bias = gaussian(streams_of[10], (D,), 0.5, 3.0, (), jnp.float32)
    grad_placed = gaussian(streams_of[11], (GROUPS * LEN, 4 * D), ((GROUPS * BLOCK) ** -0.5), 0.026977539, ((0, 768),))
    return {"patches": patches, "clip_tokens": clip_tokens, "positions": positions, "norm_gain": norm_gain, "norm_bias": norm_bias, "w_qkv": w_qkv, "b_qkv": b_qkv, "w_proj": w_proj, "b_proj": b_proj, "merge_gain": merge_gain, "merge_bias": merge_bias, "grad_placed": grad_placed}


EPSILON = 1e-06

def lowered(values):
    return lax.optimization_barrier(values.astype(jnp.bfloat16))

def normalize(values, gain_row, bias_row):
    center = values - lax.optimization_barrier(jnp.mean(values, axis=-1, keepdims=True))
    inverse = lax.rsqrt(lax.optimization_barrier(jnp.mean(center * center, axis=-1, keepdims=True)) + EPSILON)
    unit_rows = center * inverse
    return (unit_rows * gain_row + bias_row, unit_rows, inverse)

def normalize_back(upstream, unit_rows, inverse, gain_row):
    scaled = upstream * gain_row
    return inverse * (scaled - lax.optimization_barrier(jnp.mean(scaled, axis=-1, keepdims=True)) - unit_rows * lax.optimization_barrier(jnp.mean(scaled * unit_rows, axis=-1, keepdims=True)))

def one_clip(patch_rows, live_count, places, grad_rows, norm_gain, norm_bias, w_qkv, b_qkv, w_proj, b_proj, merge_gain, merge_bias):
    widened = patch_rows.astype(jnp.float32)
    normed = normalize(widened, norm_gain, norm_bias)[0].astype(jnp.bfloat16)
    triple = jnp.dot(normed, w_qkv.reshape(D, 3 * D), preferred_element_type=jnp.float32).reshape(BLOCK, 3, D) + b_qkv
    triple = lowered(triple)
    query_rows = triple[:, 0].reshape(BLOCK, HEADS, HEAD).astype(jnp.float32)
    key_rows = triple[:, 1].reshape(BLOCK, HEADS, HEAD).astype(jnp.float32)
    value_rows = triple[:, 2].reshape(BLOCK, HEADS, HEAD).astype(jnp.float32)
    scaling = HEAD ** (-0.5)
    scores = jnp.einsum('qhd,khd->hqk', query_rows, key_rows) * scaling
    live_keys = jnp.arange(BLOCK, dtype=jnp.int32) < 4 * live_count
    scores = jnp.where(live_keys[None, None, :], scores, -1e+30)
    highest = lax.optimization_barrier(jnp.max(scores, axis=-1, keepdims=True))
    powers = jnp.exp(scores - highest)
    weights = powers / lax.optimization_barrier(jnp.sum(powers, axis=-1, keepdims=True))
    weights_low = lowered(weights).astype(jnp.float32)
    attended = jnp.einsum('hqk,khd->qhd', weights_low, value_rows).reshape(BLOCK, D).astype(jnp.bfloat16)
    output = jnp.dot(attended, w_proj, preferred_element_type=jnp.float32) + b_proj + widened
    merged_full, unit_rows, inverse = normalize(output, merge_gain, merge_bias)
    merged = merged_full.reshape(BLOCK // 4, 4 * D).astype(jnp.bfloat16)
    live_tokens = jnp.arange(BLOCK // 4, dtype=jnp.int32) < live_count
    window_rows = jnp.arange(LEN, dtype=jnp.int32)
    selector = ((places[None, :] == window_rows[:, None]) & live_tokens[None, :]).astype(jnp.bfloat16)
    placed = jnp.dot(selector, merged, preferred_element_type=jnp.float32).astype(jnp.bfloat16)
    token_grad = jnp.dot(selector.T, grad_rows, preferred_element_type=jnp.float32)
    upstream = token_grad.reshape(BLOCK, D)
    row_grad = normalize_back(upstream, unit_rows, inverse, merge_gain).astype(jnp.bfloat16)
    attn_grad = lowered(jnp.dot(row_grad, w_proj.T, preferred_element_type=jnp.float32))
    attn_grad = attn_grad.reshape(BLOCK, HEADS, HEAD).astype(jnp.float32)
    prob_grad = jnp.einsum('qhd,khd->hqk', attn_grad, value_rows)
    value_grad = jnp.einsum('hqk,qhd->khd', weights_low, attn_grad)
    score_grad = weights * (prob_grad - lax.optimization_barrier(jnp.sum(prob_grad * weights, axis=-1, keepdims=True))) * scaling
    score_grad = lowered(score_grad).astype(jnp.float32)
    query_grad = jnp.einsum('hqk,khd->qhd', score_grad, key_rows)
    key_grad = jnp.einsum('hqk,qhd->khd', score_grad, query_rows)
    triple_grad = jnp.stack([query_grad, key_grad, value_grad], axis=1).reshape(BLOCK, 3 * D).astype(jnp.bfloat16)
    contribution = lax.dot_general(normed, triple_grad, (((0,), (0,)), ((), ())), preferred_element_type=jnp.float32)
    return (placed, contribution)

def reference(patches, clip_tokens, positions, norm_gain, norm_bias, w_qkv, b_qkv, w_proj, b_proj, merge_gain, merge_bias, grad_placed):
    groups = clip_tokens.shape[0]
    clip_rows = patches.reshape(groups, BLOCK, D)
    window_grads = grad_placed.reshape(groups, LEN, 4 * D)

    def advance(running, sliced):
        patch_rows, live_count, places, grad_rows = sliced
        placed, contribution = one_clip(patch_rows, live_count, places, grad_rows, norm_gain, norm_bias, w_qkv, b_qkv, w_proj, b_proj, merge_gain, merge_bias)
        return (running + contribution, placed)
    running, placed = lax.scan(advance, jnp.zeros((D, 3 * D), jnp.float32), (clip_rows, clip_tokens, positions, window_grads))
    placed = placed.reshape(groups * LEN, 4 * D)
    grad_qkv = running.reshape(D, 3, N_SEQ, D // N_SEQ).transpose(2, 1, 3, 0).reshape(N_SEQ, 3 * (D // N_SEQ), D)
    return (placed, grad_qkv)
```

```python
import functools

import jax
import jax.numpy as jnp
import numpy as np
from jax import lax
from jax.experimental import pallas as pl
from jax.experimental.pallas import tpu as pltpu
from jax.sharding import PartitionSpec as P

HEAD = 80
MESH = pl.DeviceIdType.MESH
EPSILON = 1e-06


def one_hot(sources, shift, width):
    lanes = lax.broadcasted_iota(jnp.int32, (sources.shape[0], width), 1)
    return (lanes == sources + shift).astype(jnp.float32).astype(jnp.bfloat16)


def up_to(count, unit):
    return -(-count // unit) * unit


class Sizes:
    def __init__(self, rows_y, rows_z, width):
        self.ny, self.nz = rows_y, rows_z
        self.rows = 10 * rows_y * rows_z
        self.ca = up_to(5 * rows_z, 16)
        self.cb = up_to(5 * rows_y, 8)
        self.wa = 6 * 128
        self.wb = width - self.wa
        self.ka, self.kb = self.wa // 128, self.wb // 128
        self.ra, self.rb = up_to(5 * self.ka, 16), up_to(5 * self.kb, 16)


def source_rows(s):
    NONE = -100000
    first = np.full((s.ny, s.ca), NONE, np.int32)
    second = np.full((s.nz, s.cb), NONE, np.int32)
    third = np.full((s.nz, s.ra), NONE, np.int32)
    fourth = np.full((s.ny, s.rb), NONE, np.int32)
    for y in range(s.ny):
        for z in range(s.nz):
            for j in range(5):
                first[y, z * 5 + j] = (y * s.nz + z) * 10 + j
                second[z, y * 5 + j] = y * s.ca + z * 5 + j
    for j in range(5):
        for k in range(s.ka):
            for z in range(s.nz):
                third[z, k * 5 + j] = k * s.ca + z * 5 + j
        for k in range(s.kb):
            for y in range(s.ny):
                fourth[y, k * 5 + j] = k * s.cb + y * 5 + j
    return [jnp.asarray(a.reshape(-1, 1)) for a in (first, second, third, fourth)]


def tiles_down(values):
    return jnp.concatenate(
        [values[:, k : k + 128] for k in range(0, values.shape[1], 128)], axis=0
    )


def near_first(count):
    return sorted(range(1, count), key=lambda k: (min(k, count - k), k))


def send(source, target, send_sem, recv_sem, clip):
    copy = pltpu.make_async_remote_copy(
        src_ref=source, dst_ref=target, send_sem=send_sem, recv_sem=recv_sem,
        device_id={"clip": clip}, device_id_type=MESH,
    )
    copy.start()
    return copy


def reduce_scratch(s, width, block):
    bf = jnp.bfloat16
    dma = pltpu.SemaphoreType.DMA
    return dict(
        give=pltpu.VMEM((s.ny * s.ca, block), bf),
        got=pltpu.VMEM((s.ny * s.ca, block), bf),
        other=pltpu.VMEM((block, width), bf),
        out_a=pltpu.VMEM((s.ny, s.ca, s.wa), bf),
        in_a=pltpu.VMEM((s.ny, s.ca, s.wa), bf),
        out_b=pltpu.VMEM((s.nz, s.cb, s.wb), bf),
        in_b=pltpu.VMEM((s.nz, s.cb, s.wb), bf),
        out_c=pltpu.VMEM((s.nz, s.ra, 128), bf),
        in_c=pltpu.VMEM((s.nz, s.ra, 128), bf),
        out_d=pltpu.VMEM((s.ny, s.rb, 128), bf),
        in_d=pltpu.VMEM((s.ny, s.rb, 128), bf),
        sp=dma((2,)), rp=dma((2,)),
        sa=dma((s.ny,)), ra=dma((s.ny,)),
        sb=dma((s.nz,)), rb=dma((s.nz,)),
        sc=dma((s.nz,)), rc=dma((s.nz,)),
        sd=dma((s.ny,)), rd=dma((s.ny,)),
    )


def place_of(s):
    me = lax.axis_index("clip")
    core = lax.rem(me, 2)
    chip = lax.div(me, 2)
    z = lax.rem(chip, s.nz)
    y = lax.div(chip, s.nz)
    return y, z, core


def clip_of(s, y, z, core):
    return (y * s.nz + z) * 2 + core


def greet(s, y, z, core):
    barrier = pltpu.get_barrier_semaphore()
    def signal(clip):
        pl.semaphore_signal(barrier, inc=1, device_id={"clip": clip}, device_id_type=MESH)
    for k in range(1, s.ny):
        signal(clip_of(s, lax.rem(y + k, s.ny), z, core))
    for k in range(1, s.nz):
        signal(clip_of(s, y, lax.rem(z + k, s.nz), core))
    signal(clip_of(s, y, z, 1 - core))
    return s.ny + s.nz - 1


def mm(left, right):
    return jnp.dot(left, right, preferred_element_type=jnp.float32)


def spread(out, arrived, send_sem, recv_sem, mine, count, clip_at):
    copies = []
    for k in near_first(count):
        to = lax.rem(mine + k, count)
        copies.append((k, send(out.at[to], arrived.at[k], send_sem.at[k], recv_sem.at[k], clip_at(to))))
    return copies


def added(out, arrived, copies, mine):
    total = out[mine].astype(jnp.float32)
    for k, copy in copies:
        copy.wait_recv()
        total = total + arrived[k].astype(jnp.float32)
    return total


def clip_sum(s, tgt, nrm_ref, first, second, third, fourth, fa_ref, fb_ref, b):
    y, z, core = place_of(s)
    bf = jnp.bfloat16
    pair = clip_of(s, y, z, 1 - core)
    b["give"][...] = mm(one_hot(first[...], 5 * (1 - core), s.rows), tgt).astype(bf)
    half = send(b["give"], b["got"], b["sp"].at[1], b["rp"].at[1], pair)
    keep = mm(one_hot(first[...], 5 * core, s.rows), tgt).astype(bf)
    b_first = mm(keep, nrm_ref[:, : s.wa])
    b_second = mm(keep, nrm_ref[:, s.wa :])
    half.wait_recv()
    got = b["got"][...]
    value = b_first + mm(got, b["other"][:, : s.wa])
    b["out_a"][...] = value.reshape(s.ny, s.ca, s.wa).astype(bf)
    in_y = lambda to: clip_of(s, to, z, core)
    in_z = lambda to: clip_of(s, y, to, core)
    copies_a = spread(b["out_a"], b["in_a"], b["sa"], b["ra"], y, s.ny, in_y)
    value = (b_second + mm(got, b["other"][:, s.wa :])).astype(bf)
    value = mm(one_hot(second[...], 0, s.ny * s.ca), value)
    b["out_b"][...] = value.reshape(s.nz, s.cb, s.wb).astype(bf)
    copies_b = spread(b["out_b"], b["in_b"], b["sb"], b["rb"], z, s.nz, in_z)
    total = tiles_down(added(b["out_a"], b["in_a"], copies_a, y)).astype(bf)
    value = mm(one_hot(third[...], 0, s.ka * s.ca), total)
    b["out_c"][...] = value.reshape(s.nz, s.ra, 128).astype(bf)
    copies_c = spread(b["out_c"], b["in_c"], b["sc"], b["rc"], z, s.nz, in_z)
    total = tiles_down(added(b["out_b"], b["in_b"], copies_b, z)).astype(bf)
    value = mm(one_hot(fourth[...], 0, s.kb * s.cb), total)
    b["out_d"][...] = value.reshape(s.ny, s.rb, 128).astype(bf)
    copies_d = spread(b["out_d"], b["in_d"], b["sd"], b["rd"], y, s.ny, in_y)
    fa_ref[...] = added(b["out_c"], b["in_c"], copies_c, z)
    fb_ref[...] = added(b["out_d"], b["in_d"], copies_d, y)
    half.wait_send()
    for copies in (copies_a, copies_b, copies_c, copies_d):
        for _, copy in copies:
            copy.wait_send()


def own_rows(s, fa, fb):
    def rows(values, tiles):
        return values[: 5 * tiles].reshape(tiles, 5, 128).transpose(1, 0, 2).reshape(5, 128 * tiles)
    return jnp.concatenate([rows(fa, s.ka), rows(fb, s.kb)], axis=1)


def reduce_kernel(s, names, tgt_ref, nrm_ref, first, second, third, fourth, fa_ref, fb_ref, *scratch):
    b = dict(zip(names, scratch))
    y, z, core = place_of(s)
    pl.semaphore_wait(pltpu.get_barrier_semaphore(), greet(s, y, z, core))
    normed = send(nrm_ref, b["other"], b["sp"].at[0], b["rp"].at[0], clip_of(s, y, z, 1 - core))
    normed.wait_recv()
    clip_sum(s, tgt_ref[...], nrm_ref, first, second, third, fourth, fa_ref, fb_ref, b)
    normed.wait_send()


def reduced(s, tgt, normed):
    block, width = normed.shape
    scratch = reduce_scratch(s, width, block)
    fa, fb = pl.pallas_call(
        functools.partial(reduce_kernel, s, tuple(scratch)),
        out_shape=(
            jax.ShapeDtypeStruct((s.ra, 128), jnp.float32),
            jax.ShapeDtypeStruct((s.rb, 128), jnp.float32),
        ),
        in_specs=[pl.BlockSpec(memory_space=pltpu.VMEM)] * 6,
        out_specs=(pl.BlockSpec(memory_space=pltpu.VMEM),) * 2,
        scratch_shapes=list(scratch.values()),
        compiler_params=pltpu.CompilerParams(
            collective_id=0, has_side_effects=True, vmem_limit_bytes=60000 * 1024
        ),
    )(tgt, normed, *source_rows(s))
    return own_rows(s, fa, fb)


def cut_along(shard, dim, devices):
    lengths = shard.shape
    parts = shard.reshape(*lengths[:dim], devices, lengths[dim] // devices, *lengths[dim + 1 :])
    return jnp.moveaxis(parts, dim, 0)


def summed_on_arrival(shard, axis, dim):
    devices = lax.axis_size(axis)
    parts = lax.all_to_all(cut_along(shard, dim, devices), axis, 0, 0, tiled=True)
    return jnp.sum(parts.astype(jnp.float32), axis=0)


def normalize(values, gain_row, bias_row):
    center = values - jnp.mean(values, axis=-1, keepdims=True)
    inverse = lax.rsqrt(jnp.mean(center * center, axis=-1, keepdims=True) + EPSILON)
    unit_rows = center * inverse
    return (unit_rows * gain_row + bias_row, unit_rows, inverse)


def normalize_back(upstream, unit_rows, inverse, gain_row):
    scaled = upstream * gain_row
    return inverse * (
        scaled
        - jnp.mean(scaled, axis=-1, keepdims=True)
        - unit_rows * jnp.mean(scaled * unit_rows, axis=-1, keepdims=True)
    )


def leading(left, right):
    return lax.dot_general(
        left, right, (((0,), (0,)), ((), ())), preferred_element_type=jnp.float32
    )


def body(
    patches,
    clip_tokens,
    positions,
    norm_gain,
    norm_bias,
    w_qkv,
    b_qkv,
    w_proj,
    b_proj,
    merge_gain,
    merge_bias,
    grad_placed,
):
    block_rows = patches.shape[0]
    model_width = patches.shape[1]
    local_width = w_qkv.shape[2]
    local_heads = local_width // HEAD
    live_count = clip_tokens[0]
    places = positions[0]
    widened = patches.astype(jnp.float32)
    normed = normalize(widened, norm_gain, norm_bias)[0].astype(jnp.bfloat16)
    triple = jnp.dot(
        normed, w_qkv.reshape(model_width, 3 * local_width), preferred_element_type=jnp.float32
    )
    triple = (triple.reshape(block_rows, 3, local_width) + b_qkv).astype(jnp.bfloat16)
    query_rows = triple[:, 0].reshape(block_rows, local_heads, HEAD)
    key_rows = triple[:, 1].reshape(block_rows, local_heads, HEAD)
    value_rows = triple[:, 2].reshape(block_rows, local_heads, HEAD)
    scaling = HEAD ** (-0.5)
    scores = (
        jnp.einsum("qhd,khd->hqk", query_rows, key_rows, preferred_element_type=jnp.float32)
        * scaling
    )
    live_keys = jnp.arange(block_rows, dtype=jnp.int32) < 4 * live_count
    scores = jnp.where(live_keys[None, None, :], scores, -1e30)
    highest = jnp.max(scores, axis=-1, keepdims=True)
    powers = jnp.exp(scores - highest)
    weights = powers / jnp.sum(powers, axis=-1, keepdims=True)
    weights_low = weights.astype(jnp.bfloat16)
    attended = jnp.einsum(
        "hqk,khd->qhd", weights_low, value_rows, preferred_element_type=jnp.float32
    )
    attended = attended.reshape(block_rows, local_width).astype(jnp.bfloat16)
    partial_value = jnp.dot(attended, w_proj, preferred_element_type=jnp.float32)
    summed_share = summed_on_arrival(partial_value.astype(jnp.bfloat16), "seq", 0)
    share_count = summed_share.shape[0]
    own_start = lax.axis_index("seq") * share_count
    own_patches = lax.dynamic_slice_in_dim(widened, own_start, share_count, 0)
    output_share = summed_share + b_proj + own_patches
    output = lax.all_gather(output_share.astype(jnp.bfloat16), "seq", axis=0, tiled=True).astype(
        output_share.dtype
    )
    merged_full, unit_rows, inverse = normalize(output, merge_gain, merge_bias)
    merged = merged_full.reshape(block_rows // 4, 4 * model_width).astype(jnp.bfloat16)
    live_tokens = jnp.arange(block_rows // 4, dtype=jnp.int32) < live_count
    share_rows = grad_placed.shape[0]
    rows_here = lax.axis_index("seq") * share_rows + jnp.arange(share_rows, dtype=jnp.int32)
    selector = ((places[None, :] == rows_here[:, None]) & live_tokens[None, :]).astype(jnp.bfloat16)
    placed = jnp.dot(selector, merged, preferred_element_type=jnp.float32).astype(jnp.bfloat16)
    every_row = lax.all_gather(grad_placed, "seq", axis=0, tiled=True)
    all_rows = jnp.arange(every_row.shape[0], dtype=jnp.int32)
    chooser = ((places[None, :] == all_rows[:, None]) & live_tokens[None, :]).astype(jnp.bfloat16)
    token_grad = leading(chooser, every_row)
    upstream = token_grad.reshape(block_rows, model_width)
    row_grad = normalize_back(upstream, unit_rows, inverse, merge_gain).astype(jnp.bfloat16)
    attn_grad = lax.dot_general(
        row_grad, w_proj, (((1,), (1,)), ((), ())), preferred_element_type=jnp.float32
    )
    attn_grad = attn_grad.astype(jnp.bfloat16).reshape(block_rows, local_heads, HEAD)
    prob_grad = jnp.einsum(
        "qhd,khd->hqk", attn_grad, value_rows, preferred_element_type=jnp.float32
    )
    value_grad = jnp.einsum(
        "hqk,qhd->khd", weights_low, attn_grad, preferred_element_type=jnp.float32
    )
    score_grad = (
        weights * (prob_grad - jnp.sum(prob_grad * weights, axis=-1, keepdims=True)) * scaling
    )
    score_grad = score_grad.astype(jnp.bfloat16)
    query_grad = jnp.einsum(
        "hqk,khd->qhd", score_grad, key_rows, preferred_element_type=jnp.float32
    )
    key_grad = jnp.einsum(
        "hqk,qhd->khd", score_grad, query_rows, preferred_element_type=jnp.float32
    )
    triple_grad = jnp.stack([query_grad, key_grad, value_grad], axis=1)
    triple_grad = triple_grad.reshape(block_rows, 3 * local_width).astype(jnp.bfloat16)
    summed = reduced(Sizes(8, 12, model_width), triple_grad.T, normed)
    return (placed, summed[None])


def solution(mesh):
    placed = (
        P("clip", None),
        P("clip"),
        P("clip", None),
        P(),
        P(),
        P(None, None, "seq"),
        P(None, "seq"),
        P("seq", None),
        P(),
        P(),
        P(),
        P(("clip", "seq"), None),
    )
    return jax.shard_map(
        body,
        mesh=mesh,
        in_specs=placed,
        out_specs=(P(("clip", "seq"), None), P("seq", "clip", None)),
        check_vma=False,
    )
```

```python
import functools

import jax
import jax.numpy as jnp
import numpy as np
from jax import lax
from jax.experimental import pallas as pl
from jax.experimental.pallas import tpu as pltpu
from jax.sharding import PartitionSpec as P

HEAD = 80
MESH = pl.DeviceIdType.MESH
EPSILON = 1e-06


def one_hot(sources, shift, width):
    lanes = lax.broadcasted_iota(jnp.int32, (sources.shape[0], width), 1)
    return (lanes == sources + shift).astype(jnp.float32).astype(jnp.bfloat16)


def up_to(count, unit):
    return -(-count // unit) * unit


class Sizes:
    def __init__(self, rows_y, rows_z, width, rows):
        self.ny, self.nz = rows_y, rows_z
        self.rows = rows
        self.per = rows // (2 * rows_y * rows_z)
        self.ca = up_to(self.per * rows_z, 16)
        self.cb = up_to(self.per * rows_y, 8)
        self.wa = 6 * 128
        self.wb = width - self.wa
        self.ka, self.kb = self.wa // 128, self.wb // 128
        self.ra, self.rb = up_to(self.per * self.ka, 16), up_to(self.per * self.kb, 16)


def source_rows(s):
    NONE = -100000
    first = np.full((s.ny, s.ca), NONE, np.int32)
    second = np.full((s.nz, s.cb), NONE, np.int32)
    third = np.full((s.nz, s.ra), NONE, np.int32)
    fourth = np.full((s.ny, s.rb), NONE, np.int32)
    n = s.per
    for j in range(n):
        for y in range(s.ny):
            for z in range(s.nz):
                first[y, z * n + j] = (y * s.nz + z) * 2 * n + j
                second[z, y * n + j] = y * s.ca + z * n + j
        for k in range(s.ka):
            for z in range(s.nz):
                third[z, k * n + j] = k * s.ca + z * n + j
        for k in range(s.kb):
            for y in range(s.ny):
                fourth[y, k * n + j] = k * s.cb + y * n + j
    return [jnp.asarray(a.reshape(-1, 1)) for a in (first, second, third, fourth)]


def tiles_down(values):
    return jnp.concatenate(
        [values[:, k : k + 128] for k in range(0, values.shape[1], 128)], axis=0
    )


def near_first(count):
    return sorted(range(1, count), key=lambda k: (min(k, count - k), k))


def send(source, target, send_sem, recv_sem, clip):
    copy = pltpu.make_async_remote_copy(
        src_ref=source, dst_ref=target, send_sem=send_sem, recv_sem=recv_sem,
        device_id={"clip": clip}, device_id_type=MESH,
    )
    copy.start()
    return copy


def reduce_scratch(s, width, block):
    bf = jnp.bfloat16
    dma = pltpu.SemaphoreType.DMA
    return dict(
        give=pltpu.VMEM((s.ny * s.ca, block), bf),
        got=pltpu.VMEM((s.ny * s.ca, block), bf),
        other=pltpu.VMEM((block, width), bf),
        out_a=pltpu.VMEM((s.ny, s.ca, s.wa), bf),
        in_a=pltpu.VMEM((s.ny, s.ca, s.wa), bf),
        out_b=pltpu.VMEM((s.nz, s.cb, s.wb), bf),
        in_b=pltpu.VMEM((s.nz, s.cb, s.wb), bf),
        out_c=pltpu.VMEM((s.nz, s.ra, 128), bf),
        in_c=pltpu.VMEM((s.nz, s.ra, 128), bf),
        out_d=pltpu.VMEM((s.ny, s.rb, 128), bf),
        in_d=pltpu.VMEM((s.ny, s.rb, 128), bf),
        sp=dma((2,)), rp=dma((2,)),
        sa=dma((s.ny,)), ra=dma((s.ny,)),
        sb=dma((s.nz,)), rb=dma((s.nz,)),
        sc=dma((s.nz,)), rc=dma((s.nz,)),
        sd=dma((s.ny,)), rd=dma((s.ny,)),
    )


def place_of(s):
    me = lax.axis_index("clip")
    core = lax.rem(me, 2)
    chip = lax.div(me, 2)
    z = lax.rem(chip, s.nz)
    y = lax.div(chip, s.nz)
    return y, z, core


def clip_of(s, y, z, core):
    return (y * s.nz + z) * 2 + core


def greet(s, y, z, core):
    barrier = pltpu.get_barrier_semaphore()
    def signal(clip):
        pl.semaphore_signal(barrier, inc=1, device_id={"clip": clip}, device_id_type=MESH)
    for k in range(1, s.ny):
        signal(clip_of(s, lax.rem(y + k, s.ny), z, core))
    for k in range(1, s.nz):
        signal(clip_of(s, y, lax.rem(z + k, s.nz), core))
    signal(clip_of(s, y, z, 1 - core))
    return s.ny + s.nz - 1


def mm(left, right):
    return jnp.dot(left, right, preferred_element_type=jnp.float32)


def spread(out, arrived, send_sem, recv_sem, mine, count, clip_at):
    copies = []
    for k in near_first(count):
        to = lax.rem(mine + k, count)
        copies.append((k, send(out.at[to], arrived.at[k], send_sem.at[k], recv_sem.at[k], clip_at(to))))
    return copies


def added(out, arrived, copies, mine):
    total = out[mine].astype(jnp.float32)
    for k, copy in copies:
        copy.wait_recv()
        total = total + arrived[k].astype(jnp.float32)
    return total


def clip_sum(s, permuted, nrm_ref, between, second, third, fourth, fa_ref, fb_ref, b):
    y, z, core = place_of(s)
    bf = jnp.bfloat16
    pair = clip_of(s, y, z, 1 - core)
    b["give"][...] = permuted(1 - core)
    half = send(b["give"], b["got"], b["sp"].at[1], b["rp"].at[1], pair)
    keep = permuted(core)
    b_first = mm(keep, nrm_ref[:, : s.wa])
    b_second = mm(keep, nrm_ref[:, s.wa :])
    half.wait_recv()
    got = b["got"][...]
    value = b_first + mm(got, b["other"][:, : s.wa])
    b["out_a"][...] = value.reshape(s.ny, s.ca, s.wa).astype(bf)
    in_y = lambda to: clip_of(s, to, z, core)
    in_z = lambda to: clip_of(s, y, to, core)
    copies_a = spread(b["out_a"], b["in_a"], b["sa"], b["ra"], y, s.ny, in_y)
    value = (b_second + mm(got, b["other"][:, s.wa :])).astype(bf)
    value = mm(one_hot(second[...], 0, s.ny * s.ca), value)
    b["out_b"][...] = value.reshape(s.nz, s.cb, s.wb).astype(bf)
    copies_b = spread(b["out_b"], b["in_b"], b["sb"], b["rb"], z, s.nz, in_z)
    between()
    total = tiles_down(added(b["out_a"], b["in_a"], copies_a, y)).astype(bf)
    value = mm(one_hot(third[...], 0, s.ka * s.ca), total)
    b["out_c"][...] = value.reshape(s.nz, s.ra, 128).astype(bf)
    copies_c = spread(b["out_c"], b["in_c"], b["sc"], b["rc"], z, s.nz, in_z)
    total = tiles_down(added(b["out_b"], b["in_b"], copies_b, z)).astype(bf)
    value = mm(one_hot(fourth[...], 0, s.kb * s.cb), total)
    b["out_d"][...] = value.reshape(s.ny, s.rb, 128).astype(bf)
    copies_d = spread(b["out_d"], b["in_d"], b["sd"], b["rd"], y, s.ny, in_y)
    fa_ref[...] = added(b["out_c"], b["in_c"], copies_c, z)
    fb_ref[...] = added(b["out_d"], b["in_d"], copies_d, y)
    half.wait_send()
    for copies in (copies_a, copies_b, copies_c, copies_d):
        for _, copy in copies:
            copy.wait_send()


def own_rows(s, fa, fb):
    def rows(values, tiles):
        return values[: s.per * tiles].reshape(tiles, s.per, 128).transpose(1, 0, 2).reshape(s.per, 128 * tiles)
    return jnp.concatenate([rows(fa, s.ka), rows(fb, s.kb)], axis=1)


def normalize(values, gain_row, bias_row):
    center = values - jnp.mean(values, axis=-1, keepdims=True)
    inverse = lax.rsqrt(jnp.mean(center * center, axis=-1, keepdims=True) + EPSILON)
    unit_rows = center * inverse
    return (unit_rows * gain_row + bias_row, unit_rows, inverse)


def normalize_back(upstream, unit_rows, inverse, gain_row):
    scaled = upstream * gain_row
    return inverse * (
        scaled
        - jnp.mean(scaled, axis=-1, keepdims=True)
        - unit_rows * jnp.mean(scaled * unit_rows, axis=-1, keepdims=True)
    )


def dims(left, right, a, b):
    return lax.dot_general(
        left, right, (((a,), (b,)), ((), ())), preferred_element_type=jnp.float32
    )


def send_seq(source, target, send_sem, recv_sem, seq):
    copy = pltpu.make_async_remote_copy(
        src_ref=source, dst_ref=target, send_sem=send_sem, recv_sem=recv_sem,
        device_id={"seq": seq}, device_id_type=MESH,
    )
    copy.start()
    return copy


def block_scratch(block, width, local, n):
    bf, f32 = jnp.bfloat16, jnp.float32
    dma = pltpu.SemaphoreType.DMA
    share = block // n
    return dict(
        normed=pltpu.VMEM((block, width), bf),
        query=pltpu.VMEM((block, local), bf),
        key_value=pltpu.VMEM((2 * local, block), bf),
        probs=pltpu.VMEM((local // HEAD, block, block), f32),
        biases=pltpu.VMEM((8, 384), f32),
        up_out=pltpu.VMEM((n, share, width), bf),
        up_in=pltpu.VMEM((n, share, width), bf),
        part_out=pltpu.VMEM((n, share, width), bf),
        part_in=pltpu.VMEM((n, share, width), bf),
        row_out=pltpu.VMEM((share, width), bf),
        row_in=pltpu.VMEM((n, share, width), bf),
        merged=pltpu.VMEM((n, share, width), bf),
        query_grad=pltpu.VMEM((block, local), bf),
        kv_grad=pltpu.VMEM((2 * local, block), f32),
        su=dma((n,)), ru=dma((n,)),
        sq=dma((n,)), rq=dma((n,)),
        sr=dma((n,)), rr=dma((n,)),
        sm=dma((n,)), rm=dma((n,)),
    )


def block_kernel(
    s, n, names, tokens, patches, positions, norm_gain, norm_bias, weights, b_qkv, w_proj,
    b_proj, merge_gain, merge_bias, grads, first, second, third, fourth,
    placed_ref, fa_ref, fb_ref, *scratch
):
    b = dict(zip(names, scratch))
    bf, f32, i32 = jnp.bfloat16, jnp.float32, jnp.int32
    block, width = patches.shape
    local = w_proj.shape[0]
    heads = local // HEAD
    share = block // n
    scaling = HEAD ** (-0.5)
    y, z, core = place_of(s)
    t = lax.axis_index("seq")
    partners = greet(s, y, z, core)
    for k in range(1, n):
        pl.semaphore_signal(
            pltpu.get_barrier_semaphore(), inc=1,
            device_id={"seq": lax.rem(t + k, n)}, device_id_type=MESH,
        )
    live = tokens[0]

    b["normed"][...] = normalize(patches[...].astype(f32), norm_gain[...], norm_bias[...])[0].astype(bf)

    spread_out = lax.broadcasted_iota(i32, (block // 4, block), 1)
    token_of = lax.broadcasted_iota(i32, (block // 4, block), 0)
    spread_out = ((spread_out >> 2) == token_of).astype(f32).astype(bf)
    places = jnp.broadcast_to(positions[...].astype(f32), (8, block // 4)).astype(bf)
    places = mm(places, spread_out)[0:1].astype(i32)
    slot = lax.broadcasted_iota(i32, (1, block), 1)
    code = jnp.where(slot < 4 * live, places * 4 + (slot & 3), -1)
    row = lax.broadcasted_iota(i32, (4 * share, block), 0)
    wanted = (t * share + lax.rem(row, share)) * 4 + lax.div(row, share)
    select = (code == wanted).astype(f32).astype(bf)
    stacked = jnp.concatenate([grads[:, q * width : (q + 1) * width] for q in range(4)], axis=0)
    b["up_out"][...] = dims(select, stacked, 0, 0).reshape(n, share, width).astype(bf)

    pl.semaphore_wait(pltpu.get_barrier_semaphore(), partners + n - 1)
    pair = clip_of(s, y, z, 1 - core)
    normed_copy = send(b["normed"], b["other"], b["sp"].at[0], b["rp"].at[0], pair)
    ups = []
    for k in (2, 1, 3):
        to = lax.rem(t + k, n)
        ups.append((k, send_seq(b["up_out"].at[to], b["up_in"].at[k], b["su"].at[k], b["ru"].at[k], to)))

    normed = b["normed"][...]
    b["query"][...] = (dims(normed, weights[:local], 1, 1) + b_qkv[0:1]).astype(bf)
    b["biases"][...] = jnp.zeros((8, 384), f32)
    b["biases"][0:2, :local] = b_qkv[1:3]
    columns = b["biases"][...].T
    for p in (0, 1):
        value = dims(weights[(1 + p) * local : (2 + p) * local], normed, 1, 1)
        b["key_value"][p * local : (p + 1) * local] = (value + columns[:local, p : p + 1]).astype(bf)

    live_keys = lax.broadcasted_iota(i32, (share, block), 1) < 4 * live
    parts = []
    own_part = None
    for k in (2, 1, 3, 0):
        to = lax.rem(t + k, n)
        rows = pl.ds(pl.multiple_of(to * share, share), share)
        queries = b["query"][rows, :]
        outs = []
        for h in range(heads):
            at = slice(h * HEAD, (h + 1) * HEAD)
            scores = mm(queries[:, at], b["key_value"][at]) * scaling
            scores = jnp.where(live_keys, scores, -1e30)
            powers = jnp.exp(scores - jnp.max(scores, axis=-1, keepdims=True))
            probs = powers * (1.0 / jnp.sum(powers, axis=-1, keepdims=True))
            b["probs"][h, rows, :] = probs
            outs.append(dims(probs.astype(bf), b["key_value"][local + h * HEAD : local + (h + 1) * HEAD], 1, 1))
        attended = jnp.concatenate(outs, axis=1).astype(bf)
        part = mm(attended, w_proj[...])
        if k == 0:
            own_part = part
        else:
            b["part_out"][k] = part.astype(bf)
            parts.append((k, send_seq(b["part_out"].at[k], b["part_in"].at[k], b["sq"].at[k], b["rq"].at[k], to)))

    own = pl.ds(pl.multiple_of(t * share, share), share)
    output = own_part + b_proj[...] + patches[own, :].astype(f32)
    for k, copy in parts:
        copy.wait_recv()
        output = output + b["part_in"][k].astype(f32)
    merged, unit_rows, inverse = normalize(output, merge_gain[...], merge_bias[...])
    upstream = b["up_out"][t].astype(f32)
    for k, copy in ups:
        copy.wait_recv()
        upstream = upstream + b["up_in"][k].astype(f32)
    b["row_out"][...] = normalize_back(upstream, unit_rows, inverse, merge_gain[...]).astype(bf)
    rows_sent, merged_sent = [], []
    for k in (2, 1, 3):
        to = lax.rem(t + k, n)
        rows_sent.append((k, send_seq(b["row_out"], b["row_in"].at[k], b["sr"].at[k], b["rr"].at[k], to)))
    b["merged"][t] = merged.astype(bf)
    for k in (2, 1, 3):
        to = lax.rem(t + k, n)
        merged_sent.append((k, send_seq(b["merged"].at[t], b["merged"].at[t], b["sm"].at[k], b["rm"].at[k], to)))

    arrivals = dict(rows_sent)
    for k in (0, 1, 3, 2):
        if k == 0:
            row_grad = b["row_out"][...]
        else:
            arrivals[k].wait_recv()
            row_grad = b["row_in"][k]
        source = lax.rem(t + n - k, n)
        rows = pl.ds(pl.multiple_of(source * share, share), share)
        attn = dims(row_grad, w_proj[...], 1, 1).astype(bf)
        queries = b["query"][rows, :]
        outs = []
        for h in range(heads):
            at = slice(h * HEAD, (h + 1) * HEAD)
            below = slice(local + h * HEAD, local + (h + 1) * HEAD)
            attn_h = attn[:, at]
            prob_grad = mm(attn_h, b["key_value"][below])
            probs = b["probs"][h, rows, :]
            value_grad = dims(attn_h, probs.astype(bf), 0, 0)
            inner = jnp.sum(prob_grad * probs, axis=-1, keepdims=True)
            score_grad = (probs * (prob_grad - inner) * scaling).astype(bf)
            outs.append(dims(score_grad, b["key_value"][at], 1, 1))
            key_grad = dims(queries[:, at], score_grad, 0, 0)
            if k == 0:
                b["kv_grad"][at] = key_grad
                b["kv_grad"][below] = value_grad
            else:
                b["kv_grad"][at] += key_grad
                b["kv_grad"][below] += value_grad
        b["query_grad"][rows, :] = jnp.concatenate(outs, axis=1).astype(bf)

    kv_grad = b["kv_grad"][...].astype(bf)

    def permuted(core_at):
        hot = one_hot(first[...], s.per * core_at, s.rows)
        return (dims(hot[:, :local], b["query_grad"][...], 1, 1) + mm(hot[:, local:], kv_grad)).astype(bf)

    def between():
        rows = []
        for k, copy in merged_sent:
            copy.wait_recv()
        every = b["merged"][...].reshape(block, width)
        value = mm(select, every).astype(bf)
        for q in range(4):
            placed_ref[:, q * width : (q + 1) * width] = value[q * share : (q + 1) * share]

    normed_copy.wait_recv()
    clip_sum(s, permuted, b["normed"], between, second, third, fourth, fa_ref, fb_ref, b)
    normed_copy.wait_send()
    for copies in (ups, parts, rows_sent, merged_sent):
        for _, copy in copies:
            copy.wait_send()


def fused(s, n, *operands):
    patches, w_proj = operands[1], operands[7]
    block, width = patches.shape
    local = w_proj.shape[0]
    scratch = block_scratch(block, width, local, n) | reduce_scratch(s, width, block)
    index = source_rows(s)
    vmem = pl.BlockSpec(memory_space=pltpu.VMEM)
    placed, fa, fb = pl.pallas_call(
        functools.partial(block_kernel, s, n, tuple(scratch)),
        out_shape=(
            jax.ShapeDtypeStruct((block // n, 4 * width), jnp.bfloat16),
            jax.ShapeDtypeStruct((s.ra, 128), jnp.float32),
            jax.ShapeDtypeStruct((s.rb, 128), jnp.float32),
        ),
        in_specs=[pl.BlockSpec(memory_space=pltpu.SMEM)] + [vmem] * (len(operands) - 1 + len(index)),
        out_specs=(vmem,) * 3,
        scratch_shapes=list(scratch.values()),
        compiler_params=pltpu.CompilerParams(
            collective_id=0, has_side_effects=True, vmem_limit_bytes=60000 * 1024
        ),
    )(*operands, *index)
    return placed, own_rows(s, fa, fb)


def body(
    rows_y, rows_z, seq,
    patches, clip_tokens, positions, norm_gain, norm_bias, w_qkv, b_qkv, w_proj, b_proj,
    merge_gain, merge_bias, grad_placed,
):
    width = patches.shape[1]
    weights = w_qkv.transpose(1, 2, 0).reshape(-1, width)
    s = Sizes(rows_y, rows_z, width, weights.shape[0])
    line = lambda v: v.reshape(1, width)
    placed, summed = fused(
        s, seq, clip_tokens, patches, positions, line(norm_gain), line(norm_bias), weights, b_qkv,
        w_proj, line(b_proj), line(merge_gain), line(merge_bias), grad_placed,
    )
    return placed, summed[None]


def build(mesh, rows_y, rows_z):
    placed = (
        P("clip", None), P("clip"), P("clip", None), P(), P(), P(None, None, "seq"),
        P(None, "seq"), P("seq", None), P(), P(), P(), P(("clip", "seq"), None),
    )
    return jax.shard_map(
        functools.partial(body, rows_y, rows_z, mesh.shape["seq"]),
        mesh=mesh,
        in_specs=placed,
        out_specs=(P(("clip", "seq"), None), P("seq", "clip", None)),
        check_vma=False,
    )


def solution(mesh):
    return build(mesh, 8, 12)
```

```python
import functools

import jax
import jax.numpy as jnp
import numpy as np
from jax import lax
from jax.experimental import pallas as pl
from jax.experimental.pallas import tpu as pltpu
from jax.sharding import PartitionSpec as P

HEAD = 80
MESH = pl.DeviceIdType.MESH
EPSILON = 1e-06


def one_hot(sources, shift, width):
    lanes = lax.broadcasted_iota(jnp.int32, (sources.shape[0], width), 1)
    return (lanes == sources + shift).astype(jnp.float32).astype(jnp.bfloat16)


def up_to(count, unit):
    return -(-count // unit) * unit


class Sizes:
    def __init__(self, rows_y, rows_z, width, rows):
        self.ny, self.nz = rows_y, rows_z
        self.rows = rows
        self.per = rows // (2 * rows_y * rows_z)
        self.ca = up_to(self.per * rows_z, 16)
        self.cb = up_to(self.per * rows_y, 8)
        self.wa = 6 * 128
        self.wb = width - self.wa
        self.ka, self.kb = self.wa // 128, self.wb // 128
        self.ra, self.rb = up_to(self.per * self.ka, 16), up_to(self.per * self.kb, 16)


def source_rows(s):
    NONE = -100000
    first = np.full((s.ny, s.ca), NONE, np.int32)
    second = np.full((s.nz, s.cb), NONE, np.int32)
    third = np.full((s.nz, s.ra), NONE, np.int32)
    fourth = np.full((s.ny, s.rb), NONE, np.int32)
    n = s.per
    for j in range(n):
        for y in range(s.ny):
            for z in range(s.nz):
                first[y, z * n + j] = (y * s.nz + z) * 2 * n + j
                second[z, y * n + j] = y * s.ca + z * n + j
        for k in range(s.ka):
            for z in range(s.nz):
                third[z, k * n + j] = k * s.ca + z * n + j
        for k in range(s.kb):
            for y in range(s.ny):
                fourth[y, k * n + j] = k * s.cb + y * n + j
    return [jnp.asarray(a.reshape(-1, 1)) for a in (first, second, third, fourth)]


def tiles_down(values):
    return jnp.concatenate(
        [values[:, k : k + 128] for k in range(0, values.shape[1], 128)], axis=0
    )


def near_first(count):
    return sorted(range(1, count), key=lambda k: (min(k, count - k), k))


def send(source, target, send_sem, recv_sem, clip):
    copy = pltpu.make_async_remote_copy(
        src_ref=source, dst_ref=target, send_sem=send_sem, recv_sem=recv_sem,
        device_id={"clip": clip}, device_id_type=MESH,
    )
    copy.start()
    return copy


def reduce_scratch(s, width, block):
    bf = jnp.bfloat16
    dma = pltpu.SemaphoreType.DMA
    return dict(
        give=pltpu.VMEM((s.ny * s.ca, block), bf),
        got=pltpu.VMEM((s.ny * s.ca, block), bf),
        other=pltpu.VMEM((block, width), bf),
        out_a=pltpu.VMEM((s.ny, s.ca, s.wa), bf),
        in_a=pltpu.VMEM((s.ny, s.ca, s.wa), bf),
        out_b=pltpu.VMEM((s.nz, s.cb, s.wb), bf),
        in_b=pltpu.VMEM((s.nz, s.cb, s.wb), bf),
        out_c=pltpu.VMEM((s.nz, s.ra, 128), bf),
        in_c=pltpu.VMEM((s.nz, s.ra, 128), bf),
        out_d=pltpu.VMEM((s.ny, s.rb, 128), bf),
        in_d=pltpu.VMEM((s.ny, s.rb, 128), bf),
        sp=dma((2,)), rp=dma((2,)),
        sa=dma((s.ny,)), ra=dma((s.ny,)),
        sb=dma((s.nz,)), rb=dma((s.nz,)),
        sc=dma((s.nz,)), rc=dma((s.nz,)),
        sd=dma((s.ny,)), rd=dma((s.ny,)),
    )


def place_of(s):
    me = lax.axis_index("clip")
    core = lax.rem(me, 2)
    chip = lax.div(me, 2)
    z = lax.rem(chip, s.nz)
    y = lax.div(chip, s.nz)
    return y, z, core


def clip_of(s, y, z, core):
    return (y * s.nz + z) * 2 + core


def greet(s, y, z, core):
    barrier = pltpu.get_barrier_semaphore()
    def signal(clip):
        pl.semaphore_signal(barrier, inc=1, device_id={"clip": clip}, device_id_type=MESH)
    for k in range(1, s.ny):
        signal(clip_of(s, lax.rem(y + k, s.ny), z, core))
    for k in range(1, s.nz):
        signal(clip_of(s, y, lax.rem(z + k, s.nz), core))
    signal(clip_of(s, y, z, 1 - core))
    return s.ny + s.nz - 1


def mm(left, right):
    return jnp.dot(left, right, preferred_element_type=jnp.float32)


def spread(out, arrived, send_sem, recv_sem, mine, count, clip_at):
    copies = []
    for k in near_first(count):
        to = lax.rem(mine + k, count)
        copies.append((k, send(out.at[to], arrived.at[k], send_sem.at[k], recv_sem.at[k], clip_at(to))))
    return copies


def added(out, arrived, copies, mine):
    total = out[mine].astype(jnp.float32)
    for k, copy in copies:
        copy.wait_recv()
        total = total + arrived[k].astype(jnp.float32)
    return total


def clip_sum(s, permuted, nrm_ref, relay, between, second, third, fourth, summed_ref, b):
    y, z, core = place_of(s)
    bf = jnp.bfloat16
    pair = clip_of(s, y, z, 1 - core)
    b["give"][...] = permuted(1 - core)
    half = send(b["give"], b["got"], b["sp"].at[1], b["rp"].at[1], pair)
    keep = permuted(core)
    b_first = mm(keep, nrm_ref[:, : s.wa])
    b_second = mm(keep, nrm_ref[:, s.wa :])
    relay()
    half.wait_recv()
    got = b["got"][...]
    value = b_first + mm(got, b["other"][:, : s.wa])
    b["out_a"][...] = value.reshape(s.ny, s.ca, s.wa).astype(bf)
    in_y = lambda to: clip_of(s, to, z, core)
    in_z = lambda to: clip_of(s, y, to, core)
    copies_a = spread(b["out_a"], b["in_a"], b["sa"], b["ra"], y, s.ny, in_y)
    value = (b_second + mm(got, b["other"][:, s.wa :])).astype(bf)
    value = mm(one_hot(second[...], 0, s.ny * s.ca), value)
    b["out_b"][...] = value.reshape(s.nz, s.cb, s.wb).astype(bf)
    copies_b = spread(b["out_b"], b["in_b"], b["sb"], b["rb"], z, s.nz, in_z)
    between()
    total = tiles_down(added(b["out_a"], b["in_a"], copies_a, y)).astype(bf)
    value = mm(one_hot(third[...], 0, s.ka * s.ca), total)
    b["out_c"][...] = value.reshape(s.nz, s.ra, 128).astype(bf)
    copies_c = spread(b["out_c"], b["in_c"], b["sc"], b["rc"], z, s.nz, in_z)
    total = tiles_down(added(b["out_b"], b["in_b"], copies_b, z)).astype(bf)
    value = mm(one_hot(fourth[...], 0, s.kb * s.cb), total)
    b["out_d"][...] = value.reshape(s.ny, s.rb, 128).astype(bf)
    copies_d = spread(b["out_d"], b["in_d"], b["sd"], b["rd"], y, s.ny, in_y)
    total = added(b["out_c"], b["in_c"], copies_c, z)
    for k in range(s.ka):
        summed_ref[0, :, k * 128 : (k + 1) * 128] = total[k * s.per : (k + 1) * s.per]
    total = added(b["out_d"], b["in_d"], copies_d, y)
    for k in range(s.kb):
        summed_ref[0, :, s.wa + k * 128 : s.wa + (k + 1) * 128] = total[k * s.per : (k + 1) * s.per]
    half.wait_send()
    for copies in (copies_a, copies_b, copies_c, copies_d):
        for _, copy in copies:
            copy.wait_send()


def normalize(values, gain_row, bias_row):
    center = values - jnp.mean(values, axis=-1, keepdims=True)
    inverse = lax.rsqrt(jnp.mean(center * center, axis=-1, keepdims=True) + EPSILON)
    unit_rows = center * inverse
    return (unit_rows * gain_row + bias_row, unit_rows, inverse)


def normalize_back(upstream, unit_rows, inverse, gain_row):
    scaled = upstream * gain_row
    return inverse * (
        scaled
        - jnp.mean(scaled, axis=-1, keepdims=True)
        - unit_rows * jnp.mean(scaled * unit_rows, axis=-1, keepdims=True)
    )


def vector(ref):
    return ref[...].reshape(1, ref.shape[0])


def dims(left, right, a, b):
    return lax.dot_general(
        left, right, (((a,), (b,)), ((), ())), preferred_element_type=jnp.float32
    )


def send_seq(source, target, send_sem, recv_sem, seq):
    copy = pltpu.make_async_remote_copy(
        src_ref=source, dst_ref=target, send_sem=send_sem, recv_sem=recv_sem,
        device_id={"seq": seq}, device_id_type=MESH,
    )
    copy.start()
    return copy


def block_scratch(block, width, local, n):
    bf, f32 = jnp.bfloat16, jnp.float32
    dma = pltpu.SemaphoreType.DMA
    share = block // n
    return dict(
        normed=pltpu.VMEM((block, width), bf),
        query=pltpu.VMEM((block, local), bf),
        key_value=pltpu.VMEM((2 * local, block), bf),
        probs=pltpu.VMEM((local // HEAD, block, block), f32),
        biases=pltpu.VMEM((8, 384), f32),
        up_out=pltpu.VMEM((n, share, width), bf),
        up_in=pltpu.VMEM((3, share, width), bf),
        part_out=pltpu.VMEM((3, share, width), bf),
        part_in=pltpu.VMEM((3, share, width), bf),
        row_out=pltpu.VMEM((share, width), bf),
        row_in=pltpu.VMEM((3, share, width), bf),
        patches=pltpu.VMEM((block, width), bf),
        weights=pltpu.VMEM((3 * local, width), bf),
        w_proj=pltpu.VMEM((local, width), bf),
        grads=pltpu.VMEM((share, 4 * width), bf),
        loads=dma((4,)),
        merged=pltpu.VMEM((n, share, width), bf),
        query_grad=pltpu.VMEM((block, local), bf),
        kv_grad=pltpu.VMEM((2 * local, block), f32),
        su=dma((3,)), ru=dma((3,)),
        sq=dma((3,)), rq=dma((3,)),
        sr=dma((3,)), rr=dma((3,)),
        sm=dma((3,)), rm=dma((3,)),
    )


def block_kernel(
    s, n, names, tokens, patches_in, positions, norm_gain, norm_bias, weights_in, b_qkv,
    w_proj_in, b_proj, merge_gain, merge_bias, grads_in, first, second, third, fourth,
    placed_ref, summed_ref, *scratch
):
    b = dict(zip(names, scratch))
    loads = []
    for i, (source, name) in enumerate(
        ((grads_in, "grads"), (patches_in, "patches"), (weights_in, "weights"), (w_proj_in, "w_proj"))
    ):
        load = pltpu.make_async_copy(source, b[name], b["loads"].at[i])
        load.start()
        loads.append(load)
    patches, weights, w_proj, grads = b["patches"], b["weights"], b["w_proj"], b["grads"]
    bf, f32, i32 = jnp.bfloat16, jnp.float32, jnp.int32
    block, width = patches.shape
    local = w_proj.shape[0]
    heads = local // HEAD
    share = block // n
    scaling = HEAD ** (-0.5)
    y, z, core = place_of(s)
    t = lax.axis_index("seq")
    ahead = lax.rem(t + 1 + 2 * core, n)
    behind = lax.rem(t + 3 - 2 * core, n)
    across = lax.rem(t + 2, n)
    partners = greet(s, y, z, core)
    for k in range(1, n):
        pl.semaphore_signal(
            pltpu.get_barrier_semaphore(), inc=1,
            device_id={"seq": lax.rem(t + k, n)}, device_id_type=MESH,
        )
    live = tokens[0]

    spread_out = lax.broadcasted_iota(i32, (block // 4, block), 1)
    token_of = lax.broadcasted_iota(i32, (block // 4, block), 0)
    spread_out = ((spread_out >> 2) == token_of).astype(f32).astype(bf)
    places = jnp.broadcast_to(positions[...].astype(f32), (8, block // 4)).astype(bf)
    places = mm(places, spread_out)[0:1].astype(i32)
    slot = lax.broadcasted_iota(i32, (1, block), 1)
    code = jnp.where(slot < 4 * live, places * 4 + (slot & 3), -1)
    row = lax.broadcasted_iota(i32, (4 * share, block), 0)
    wanted = (t * share + lax.rem(row, share)) * 4 + lax.div(row, share)
    select = (code == wanted).astype(f32).astype(bf)
    loads[0].wait()
    stacked = jnp.concatenate([grads[:, q * width : (q + 1) * width] for q in range(4)], axis=0)
    b["up_out"][...] = dims(select, stacked, 0, 0).reshape(n, share, width).astype(bf)
    loads[1].wait()
    b["normed"][...] = normalize(patches[...].astype(f32), vector(norm_gain), vector(norm_bias))[0].astype(bf)

    pl.semaphore_wait(pltpu.get_barrier_semaphore(), partners + n - 1)
    pair = clip_of(s, y, z, 1 - core)
    normed_copy = send(b["normed"], b["other"], b["sp"].at[0], b["rp"].at[0], pair)
    def pass_on(out, arrived, sends, arrivals, i, to):
        return send_seq(out, arrived.at[i], b[sends].at[i], b[arrivals].at[i], to)

    ups = [
        pass_on(b["up_out"].at[across], b["up_in"], "su", "ru", 0, ahead),
        pass_on(b["up_out"].at[behind], b["up_in"], "su", "ru", 1, behind),
    ]
    loads[2].wait()
    normed = b["normed"][...]
    b["query"][...] = (dims(normed, weights[:local], 1, 1) + b_qkv[0:1]).astype(bf)
    b["biases"][...] = jnp.zeros((8, 384), f32)
    b["biases"][0:2, :local] = b_qkv[1:3]
    columns = b["biases"][...].T
    for p in (0, 1):
        value = dims(weights[(1 + p) * local : (2 + p) * local], normed, 1, 1)
        b["key_value"][p * local : (p + 1) * local] = (value + columns[:local, p : p + 1]).astype(bf)

    ups[0].wait_recv()
    b["up_out"][ahead] = (b["up_out"][ahead].astype(f32) + b["up_in"][0].astype(f32)).astype(bf)
    ups.append(pass_on(b["up_out"].at[ahead], b["up_in"], "su", "ru", 2, ahead))

    live_keys = lax.broadcasted_iota(i32, (share, block), 1) < 4 * live
    loads[3].wait()
    parts = []

    def attend(to):
        rows = pl.ds(pl.multiple_of(to * share, share), share)
        queries = b["query"][rows, :]
        outs = []
        for h in range(heads):
            at = slice(h * HEAD, (h + 1) * HEAD)
            scores = mm(queries[:, at], b["key_value"][at]) * scaling
            scores = jnp.where(live_keys, scores, -1e30)
            powers = jnp.exp(scores - jnp.max(scores, axis=-1, keepdims=True))
            probs = powers * (1.0 / jnp.sum(powers, axis=-1, keepdims=True))
            b["probs"][h, rows, :] = probs
            outs.append(dims(probs.astype(bf), b["key_value"][local + h * HEAD : local + (h + 1) * HEAD], 1, 1))
        attended = jnp.concatenate(outs, axis=1).astype(bf)
        return mm(attended, w_proj[...])

    b["part_out"][0] = attend(across).astype(bf)
    parts.append(pass_on(b["part_out"].at[0], b["part_in"], "sq", "rq", 0, ahead))
    b["part_out"][1] = attend(behind).astype(bf)
    parts.append(pass_on(b["part_out"].at[1], b["part_in"], "sq", "rq", 1, behind))
    part = attend(ahead)
    parts[0].wait_recv()
    b["part_out"][2] = (part + b["part_in"][0].astype(f32)).astype(bf)
    parts.append(pass_on(b["part_out"].at[2], b["part_in"], "sq", "rq", 2, ahead))
    own = pl.ds(pl.multiple_of(t * share, share), share)
    output = attend(t) + vector(b_proj) + patches[own, :].astype(f32)
    upstream = b["up_out"][t].astype(f32)
    for i in (1, 2):
        ups[i].wait_recv()
        upstream = upstream + b["up_in"][i].astype(f32)
    for i in (1, 2):
        parts[i].wait_recv()
        output = output + b["part_in"][i].astype(f32)
    merged, unit_rows, inverse = normalize(output, vector(merge_gain), vector(merge_bias))
    b["row_out"][...] = normalize_back(upstream, unit_rows, inverse, vector(merge_gain)).astype(bf)
    rows_sent = [
        pass_on(b["row_out"], b["row_in"], "sr", "rr", 0, ahead),
        pass_on(b["row_out"], b["row_in"], "sr", "rr", 1, behind),
    ]
    b["merged"][t] = merged.astype(bf)

    for k, source in enumerate((t, behind, ahead, across)):
        if k == 0:
            row_grad = b["row_out"][...]
        else:
            rows_sent[k - 1].wait_recv()
            row_grad = b["row_in"][k - 1]
        if k == 1:
            rows_sent.append(pass_on(b["row_in"].at[0], b["row_in"], "sr", "rr", 2, ahead))
        if k == 3:
            merged_sent = [
                send_seq(b["merged"].at[t], b["merged"].at[t], b["sm"].at[i], b["rm"].at[i], to)
                for i, to in enumerate((ahead, behind))
            ]
        rows = pl.ds(pl.multiple_of(source * share, share), share)
        attn = dims(row_grad, w_proj[...], 1, 1).astype(bf)
        queries = b["query"][rows, :]
        outs = []
        for h in range(heads):
            at = slice(h * HEAD, (h + 1) * HEAD)
            below = slice(local + h * HEAD, local + (h + 1) * HEAD)
            attn_h = attn[:, at]
            prob_grad = mm(attn_h, b["key_value"][below])
            probs = b["probs"][h, rows, :]
            value_grad = dims(attn_h, probs.astype(bf), 0, 0)
            inner = jnp.sum(prob_grad * probs, axis=-1, keepdims=True)
            score_grad = (probs * (prob_grad - inner) * scaling).astype(bf)
            outs.append(dims(score_grad, b["key_value"][at], 1, 1))
            key_grad = dims(queries[:, at], score_grad, 0, 0)
            if k == 0:
                b["kv_grad"][at] = key_grad
                b["kv_grad"][below] = value_grad
            else:
                b["kv_grad"][at] += key_grad
                b["kv_grad"][below] += value_grad
        b["query_grad"][rows, :] = jnp.concatenate(outs, axis=1).astype(bf)

    kv_grad = b["kv_grad"][...].astype(bf)

    def permuted(core_at):
        hot = one_hot(first[...], s.per * core_at, s.rows)
        return (dims(hot[:, :local], b["query_grad"][...], 1, 1) + mm(hot[:, local:], kv_grad)).astype(bf)

    def relay():
        merged_sent[0].wait_recv()
        merged_sent.append(
            send_seq(b["merged"].at[behind], b["merged"].at[behind], b["sm"].at[2], b["rm"].at[2], ahead)
        )

    def between():
        for copy in merged_sent[1:]:
            copy.wait_recv()
        every = b["merged"][...].reshape(block, width)
        value = mm(select, every).astype(bf)
        for q in range(4):
            placed_ref[:, q * width : (q + 1) * width] = value[q * share : (q + 1) * share]

    normed_copy.wait_recv()
    clip_sum(s, permuted, b["normed"], relay, between, second, third, fourth, summed_ref, b)
    normed_copy.wait_send()
    for copies in (ups, parts, rows_sent, merged_sent):
        for copy in copies:
            copy.wait_send()


def fused(s, n, *operands):
    patches, w_proj = operands[1], operands[7]
    block, width = patches.shape
    local = w_proj.shape[0]
    scratch = block_scratch(block, width, local, n) | reduce_scratch(s, width, block)
    index = source_rows(s)
    vmem = pl.BlockSpec(memory_space=pltpu.VMEM)
    anywhere = pl.BlockSpec(memory_space=pl.ANY)
    specs = [vmem] * (len(operands) + len(index))
    specs[0] = pl.BlockSpec(memory_space=pltpu.SMEM)
    for i in (1, 5, 7, 11):
        specs[i] = anywhere
    return pl.pallas_call(
        functools.partial(block_kernel, s, n, tuple(scratch)),
        out_shape=(
            jax.ShapeDtypeStruct((block // n, 4 * width), jnp.bfloat16),
            jax.ShapeDtypeStruct((1, s.per, width), jnp.float32),
        ),
        in_specs=specs,
        out_specs=(vmem,) * 2,
        scratch_shapes=list(scratch.values()),
        compiler_params=pltpu.CompilerParams(
            collective_id=0, has_side_effects=True, vmem_limit_bytes=60000 * 1024
        ),
    )(*operands, *index)


def body(
    rows_y, rows_z, seq,
    patches, clip_tokens, positions, norm_gain, norm_bias, w_qkv, b_qkv, w_proj, b_proj,
    merge_gain, merge_bias, grad_placed,
):
    width = patches.shape[1]
    weights = w_qkv.transpose(1, 2, 0).reshape(-1, width)
    s = Sizes(rows_y, rows_z, width, weights.shape[0])
    return fused(
        s, seq, clip_tokens, patches, positions, norm_gain, norm_bias, weights, b_qkv,
        w_proj, b_proj, merge_gain, merge_bias, grad_placed,
    )


def build(mesh, rows_y, rows_z):
    placed = (
        P("clip", None), P("clip"), P("clip", None), P(), P(), P(None, None, "seq"),
        P(None, "seq"), P("seq", None), P(), P(), P(), P(("clip", "seq"), None),
    )
    return jax.shard_map(
        functools.partial(body, rows_y, rows_z, mesh.shape["seq"]),
        mesh=mesh,
        in_specs=placed,
        out_specs=(P(("clip", "seq"), None), P("seq", "clip", None)),
        check_vma=False,
    )


def solution(mesh):
    return build(mesh, 8, 12)
```

```python
import functools

import jax
import jax.numpy as jnp
import numpy as np
from jax import lax
from jax.experimental import pallas as pl
from jax.experimental.pallas import tpu as pltpu
from jax.sharding import PartitionSpec as P

HEAD = 80
MESH = pl.DeviceIdType.MESH
EPSILON = 1e-06


def one_hot(sources, shift, width):
    lanes = lax.broadcasted_iota(jnp.int32, (sources.shape[0], width), 1)
    return (lanes == sources + shift).astype(jnp.float32).astype(jnp.bfloat16)


def up_to(count, unit):
    return -(-count // unit) * unit


class Sizes:
    def __init__(self, rows_y, rows_z, width, rows):
        self.ny, self.nz = rows_y // 2, rows_z // 2
        self.rows = rows
        self.per = rows // (2 * rows_y * rows_z)
        self.ca = up_to(self.per * self.nz, 16)
        self.cb = up_to(self.per * self.ny, 8)
        self.wa = 6 * 128
        self.wb = width - self.wa
        self.ka, self.kb = self.wa // 128, self.wb // 128
        self.ra, self.rb = up_to(self.per * self.ka, 16), up_to(self.per * self.kb, 16)


def source_rows(groups, length, count, unit, steps):
    row = lax.broadcasted_iota(jnp.int32, (groups * length, 1), 0)
    group, inside = lax.div(row, length), lax.rem(row, length)
    major, minor = lax.div(inside, unit), lax.rem(inside, unit)
    source = group * steps[0] + major * steps[1] + minor
    return jnp.where(inside < count * unit, source, -100000)


def first_rows(s):
    return source_rows(s.ny, s.ca, s.nz, s.per, (8 * s.per * s.nz, 4 * s.per))


def second_rows(s):
    return source_rows(s.nz, s.cb, s.ny, s.per, (s.per, s.ca))


def third_rows(s):
    return source_rows(s.nz, s.ra, s.ka, s.per, (s.per, s.ca))


def fourth_rows(s):
    return source_rows(s.ny, s.rb, s.kb, s.per, (s.per, s.cb))


def tiles_down(values):
    return jnp.concatenate(
        [values[:, k : k + 128] for k in range(0, values.shape[1], 128)], axis=0
    )


def near_first(count):
    return sorted(range(1, count), key=lambda k: (min(k, count - k), k))


def send(source, target, send_sem, recv_sem, clip):
    copy = pltpu.make_async_remote_copy(
        src_ref=source, dst_ref=target, send_sem=send_sem, recv_sem=recv_sem,
        device_id={"clip": clip}, device_id_type=MESH,
    )
    copy.start()
    return copy


def reduce_scratch(s, width, block):
    bf = jnp.bfloat16
    dma = pltpu.SemaphoreType.DMA
    return dict(
        give=pltpu.VMEM((8, s.ny * s.ca, block), bf),
        got=pltpu.VMEM((8, s.ny * s.ca, block), bf),
        others=pltpu.VMEM((8, block, width), bf),
        out_a=pltpu.VMEM((s.ny, s.ca, s.wa), bf),
        in_a=pltpu.VMEM((s.ny, s.ca, s.wa), bf),
        out_b=pltpu.VMEM((s.nz, s.cb, s.wb), bf),
        in_b=pltpu.VMEM((s.nz, s.cb, s.wb), bf),
        out_c=pltpu.VMEM((s.nz, s.ra, 128), bf),
        in_c=pltpu.VMEM((s.nz, s.ra, 128), bf),
        out_d=pltpu.VMEM((s.ny, s.rb, 128), bf),
        in_d=pltpu.VMEM((s.ny, s.rb, 128), bf),
        sn=dma((8,)), rn=dma((8,)),
        sp=dma((8,)), rp=dma((8,)),
        sa=dma((s.ny,)), ra=dma((s.ny,)),
        sb=dma((s.nz,)), rb=dma((s.nz,)),
        sc=dma((s.nz,)), rc=dma((s.nz,)),
        sd=dma((s.ny,)), rd=dma((s.ny,)),
    )


def place_of(s):
    me = lax.axis_index("clip")
    core = lax.rem(me, 2)
    chip = lax.div(me, 2)
    z = lax.rem(chip, 2 * s.nz)
    y = lax.div(chip, 2 * s.nz)
    return lax.div(y, 2), lax.div(z, 2), lax.rem(y, 2), lax.rem(z, 2), core


def clip_of(s, place):
    y, z, odd_y, odd_z, core = place
    return ((2 * y + odd_y) * 2 * s.nz + 2 * z + odd_z) * 2 + core


def flipped(place, k):
    y, z, *bits = place
    return (y, z, *(1 - bit if k & (4 >> i) else bit for i, bit in enumerate(bits)))


def along_y(place, count, k):
    return (lax.rem(place[0] + k, count),) + place[1:]


def along_z(place, count, k):
    return (place[0], lax.rem(place[1] + k, count)) + place[2:]


def greet(s, place):
    barrier = pltpu.get_barrier_semaphore()
    others = [flipped(place, k) for k in range(1, 8)]
    others += [along_y(place, s.ny, k) for k in range(1, s.ny)]
    others += [along_z(place, s.nz, k) for k in range(1, s.nz)]
    for other in others:
        pl.semaphore_signal(
            barrier, inc=1, device_id={"clip": clip_of(s, other)}, device_id_type=MESH
        )
    return len(others)


def mm(left, right):
    return jnp.dot(left, right, preferred_element_type=jnp.float32)


def spread(s, out, arrived, send_sem, recv_sem, place, dim):
    along, count = ((along_y, s.ny), (along_z, s.nz))[dim]
    copies = []
    for k in near_first(count):
        other = along(place, count, k)
        copies.append((k, send(
            out.at[other[dim]], arrived.at[k], send_sem.at[k], recv_sem.at[k], clip_of(s, other)
        )))
    return copies


def added(out, arrived, copies, mine):
    total = out[mine].astype(jnp.float32)
    for k, copy in copies:
        copy.wait_recv()
        total = total + arrived[k].astype(jnp.float32)
    return total


def share_normed(s, place, b):
    copies = {}
    for k in (6, 4, 2, 1):
        copies[k] = send(
            b["normed"], b["others"].at[k], b["sn"].at[k], b["rn"].at[k], clip_of(s, flipped(place, k))
        )
    return copies


def clip_sum(s, place, permuted, normed, relay, between, summed_ref, b):
    y, z = place[:2]
    bf = jnp.bfloat16

    def rows_for(other):
        return permuted(((other[2] * 2 * s.nz + other[3]) * 2 + other[4]) * s.per)

    given = {}
    for k in (6, 7, 4, 5, 2, 3, 1):
        other = flipped(place, k)
        b["give"][k] = rows_for(other)
        given[k] = send(b["give"].at[k], b["got"].at[k], b["sp"].at[k], b["rp"].at[k], clip_of(s, other))
    pair = clip_of(s, flipped(place, 1))
    for k in (2, 4, 6):
        normed[k].wait_recv()
        normed[k + 1] = send(
            b["others"].at[k], b["others"].at[k + 1], b["sn"].at[k + 1], b["rn"].at[k + 1], pair
        )
    value = mm(rows_for(place), b["normed"][...])
    relay()
    for k in (1, 2, 4, 3, 5, 6, 7):
        if k & 1:
            normed[k].wait_recv()
        given[k].wait_recv()
        value = value + mm(b["got"][k], b["others"][k])
    b["out_a"][...] = value[:, : s.wa].reshape(s.ny, s.ca, s.wa).astype(bf)
    copies_a = spread(s, b["out_a"], b["in_a"], b["sa"], b["ra"], place, 0)
    value = mm(one_hot(second_rows(s), 0, s.ny * s.ca), value[:, s.wa :].astype(bf))
    b["out_b"][...] = value.reshape(s.nz, s.cb, s.wb).astype(bf)
    copies_b = spread(s, b["out_b"], b["in_b"], b["sb"], b["rb"], place, 1)
    between()
    total = tiles_down(added(b["out_a"], b["in_a"], copies_a, y)).astype(bf)
    value = mm(one_hot(third_rows(s), 0, s.ka * s.ca), total)
    b["out_c"][...] = value.reshape(s.nz, s.ra, 128).astype(bf)
    copies_c = spread(s, b["out_c"], b["in_c"], b["sc"], b["rc"], place, 1)
    total = tiles_down(added(b["out_b"], b["in_b"], copies_b, z)).astype(bf)
    value = mm(one_hot(fourth_rows(s), 0, s.kb * s.cb), total)
    b["out_d"][...] = value.reshape(s.ny, s.rb, 128).astype(bf)
    copies_d = spread(s, b["out_d"], b["in_d"], b["sd"], b["rd"], place, 0)
    total = added(b["out_c"], b["in_c"], copies_c, z)
    for k in range(s.ka):
        summed_ref[:, 0, k * 128 : (k + 1) * 128] = total[k * s.per : (k + 1) * s.per]
    total = added(b["out_d"], b["in_d"], copies_d, y)
    for k in range(s.kb):
        summed_ref[:, 0, s.wa + k * 128 : s.wa + (k + 1) * 128] = total[k * s.per : (k + 1) * s.per]
    for copies in (normed, given):
        for copy in copies.values():
            copy.wait_send()
    for copies in (copies_a, copies_b, copies_c, copies_d):
        for _, copy in copies:
            copy.wait_send()


def normalize(values, gain_row, bias_row):
    center = values - jnp.mean(values, axis=-1, keepdims=True)
    inverse = lax.rsqrt(jnp.mean(center * center, axis=-1, keepdims=True) + EPSILON)
    unit_rows = center * inverse
    return (unit_rows * gain_row + bias_row, unit_rows, inverse)


def normalize_back(upstream, unit_rows, inverse, gain_row):
    scaled = upstream * gain_row
    return inverse * (
        scaled
        - jnp.mean(scaled, axis=-1, keepdims=True)
        - unit_rows * jnp.mean(scaled * unit_rows, axis=-1, keepdims=True)
    )


def vector(ref):
    return ref[...].reshape(1, ref.shape[0])


def dims(left, right, a, b):
    return lax.dot_general(
        left, right, (((a,), (b,)), ((), ())), preferred_element_type=jnp.float32
    )


def send_seq(source, target, send_sem, recv_sem, seq):
    copy = pltpu.make_async_remote_copy(
        src_ref=source, dst_ref=target, send_sem=send_sem, recv_sem=recv_sem,
        device_id={"seq": seq}, device_id_type=MESH,
    )
    copy.start()
    return copy


def block_scratch(block, width, local, n):
    bf, f32 = jnp.bfloat16, jnp.float32
    dma = pltpu.SemaphoreType.DMA
    share = block // n
    return dict(
        normed=pltpu.VMEM((block, width), bf),
        query=pltpu.VMEM((block, local), bf),
        key_value=pltpu.VMEM((2 * local, block), bf),
        probs=pltpu.VMEM((local // HEAD, block, block), f32),
        biases=pltpu.VMEM((8, 384), f32),
        up_out=pltpu.VMEM((n, share, width), bf),
        up_in=pltpu.VMEM((3, share, width), bf),
        part_out=pltpu.VMEM((3, share, width), bf),
        part_in=pltpu.VMEM((3, share, width), bf),
        row_out=pltpu.VMEM((share, width), bf),
        row_in=pltpu.VMEM((3, share, width), bf),
        patches=pltpu.VMEM((block, width), bf),
        weights=pltpu.VMEM((3 * local, width), bf),
        w_proj=pltpu.VMEM((local, width), bf),
        grads=pltpu.VMEM((share, 4 * width), bf),
        loads=dma((4,)),
        merged=pltpu.VMEM((n, share, width), bf),
        query_grad=pltpu.VMEM((block, local), bf),
        kv_grad=pltpu.VMEM((2 * local, block), f32),
        su=dma((3,)), ru=dma((3,)),
        sq=dma((3,)), rq=dma((3,)),
        sr=dma((3,)), rr=dma((3,)),
        sm=dma((3,)), rm=dma((3,)),
    )


def block_kernel(
    s, n, names, tokens, patches_in, positions, norm_gain, norm_bias, weights_in, b_qkv,
    w_proj_in, b_proj, merge_gain, merge_bias, grads_in,
    placed_ref, summed_ref, *scratch
):
    b = dict(zip(names, scratch))
    loads = []
    for i, (source, name) in enumerate(
        ((grads_in, "grads"), (patches_in, "patches"), (weights_in, "weights"), (w_proj_in, "w_proj"))
    ):
        load = pltpu.make_async_copy(source, b[name], b["loads"].at[i])
        load.start()
        loads.append(load)
    patches, weights, w_proj, grads = b["patches"], b["weights"], b["w_proj"], b["grads"]
    bf, f32, i32 = jnp.bfloat16, jnp.float32, jnp.int32
    block, width = patches.shape
    local = w_proj.shape[0]
    heads = local // HEAD
    share = block // n
    scaling = HEAD ** (-0.5)
    place = place_of(s)
    core = place[4]
    t = lax.axis_index("seq")
    ahead = lax.rem(t + 1 + 2 * core, n)
    behind = lax.rem(t + 3 - 2 * core, n)
    across = lax.rem(t + 2, n)
    partners = greet(s, place)
    for k in range(1, n):
        pl.semaphore_signal(
            pltpu.get_barrier_semaphore(), inc=1,
            device_id={"seq": lax.rem(t + k, n)}, device_id_type=MESH,
        )
    live = tokens[0]

    spread_out = lax.broadcasted_iota(i32, (block // 4, block), 1)
    token_of = lax.broadcasted_iota(i32, (block // 4, block), 0)
    spread_out = ((spread_out >> 2) == token_of).astype(f32).astype(bf)
    places = jnp.broadcast_to(positions[...].astype(f32), (8, block // 4)).astype(bf)
    places = mm(places, spread_out)[0:1].astype(i32)
    slot = lax.broadcasted_iota(i32, (1, block), 1)
    code = jnp.where(slot < 4 * live, places * 4 + (slot & 3), -1)
    row = lax.broadcasted_iota(i32, (4 * share, block), 0)
    wanted = (t * share + lax.rem(row, share)) * 4 + lax.div(row, share)
    select = (code == wanted).astype(f32).astype(bf)
    loads[0].wait()
    stacked = jnp.concatenate([grads[:, q * width : (q + 1) * width] for q in range(4)], axis=0)
    b["up_out"][...] = dims(select, stacked, 0, 0).reshape(n, share, width).astype(bf)
    loads[1].wait()
    b["normed"][...] = normalize(patches[...].astype(f32), vector(norm_gain), vector(norm_bias))[0].astype(bf)

    pl.semaphore_wait(pltpu.get_barrier_semaphore(), partners + n - 1)
    def pass_on(out, arrived, sends, arrivals, i, to):
        return send_seq(out, arrived.at[i], b[sends].at[i], b[arrivals].at[i], to)

    ups = [
        pass_on(b["up_out"].at[across], b["up_in"], "su", "ru", 0, ahead),
        pass_on(b["up_out"].at[behind], b["up_in"], "su", "ru", 1, behind),
    ]
    shared = share_normed(s, place, b)
    loads[2].wait()
    normed = b["normed"][...]
    b["query"][...] = (dims(normed, weights[:local], 1, 1) + b_qkv[0:1]).astype(bf)
    b["biases"][...] = jnp.zeros((8, 384), f32)
    b["biases"][0:2, :local] = b_qkv[1:3]
    columns = b["biases"][...].T
    for p in (0, 1):
        value = dims(weights[(1 + p) * local : (2 + p) * local], normed, 1, 1)
        b["key_value"][p * local : (p + 1) * local] = (value + columns[:local, p : p + 1]).astype(bf)

    live_keys = lax.broadcasted_iota(i32, (share, block), 1) < 4 * live
    loads[3].wait()
    parts = []

    def attend(to):
        rows = pl.ds(pl.multiple_of(to * share, share), share)
        queries = b["query"][rows, :]
        outs = []
        for h in range(heads):
            at = slice(h * HEAD, (h + 1) * HEAD)
            scores = mm(queries[:, at], b["key_value"][at]) * scaling
            scores = jnp.where(live_keys, scores, -1e30)
            powers = jnp.exp(scores - jnp.max(scores, axis=-1, keepdims=True))
            probs = powers * (1.0 / jnp.sum(powers, axis=-1, keepdims=True))
            b["probs"][h, rows, :] = probs
            outs.append(dims(probs.astype(bf), b["key_value"][local + h * HEAD : local + (h + 1) * HEAD], 1, 1))
        attended = jnp.concatenate(outs, axis=1).astype(bf)
        return mm(attended, w_proj[...])

    b["part_out"][0] = attend(across).astype(bf)
    parts.append(pass_on(b["part_out"].at[0], b["part_in"], "sq", "rq", 0, ahead))
    b["part_out"][1] = attend(behind).astype(bf)
    parts.append(pass_on(b["part_out"].at[1], b["part_in"], "sq", "rq", 1, behind))
    ups[0].wait_recv()
    b["up_out"][ahead] = (b["up_out"][ahead].astype(f32) + b["up_in"][0].astype(f32)).astype(bf)
    ups.append(pass_on(b["up_out"].at[ahead], b["up_in"], "su", "ru", 2, ahead))
    part = attend(ahead)
    parts[0].wait_recv()
    b["part_out"][2] = (part + b["part_in"][0].astype(f32)).astype(bf)
    parts.append(pass_on(b["part_out"].at[2], b["part_in"], "sq", "rq", 2, ahead))
    own = pl.ds(pl.multiple_of(t * share, share), share)
    output = attend(t) + vector(b_proj) + patches[own, :].astype(f32)
    upstream = b["up_out"][t].astype(f32)
    for i in (1, 2):
        ups[i].wait_recv()
        upstream = upstream + b["up_in"][i].astype(f32)
    for i in (1, 2):
        parts[i].wait_recv()
        output = output + b["part_in"][i].astype(f32)
    merged, unit_rows, inverse = normalize(output, vector(merge_gain), vector(merge_bias))
    b["row_out"][...] = normalize_back(upstream, unit_rows, inverse, vector(merge_gain)).astype(bf)
    rows_sent = [
        pass_on(b["row_out"], b["row_in"], "sr", "rr", 0, ahead),
        pass_on(b["row_out"], b["row_in"], "sr", "rr", 1, behind),
    ]
    b["merged"][t] = merged.astype(bf)

    for k, source in enumerate((t, behind, ahead, across)):
        if k == 0:
            row_grad = b["row_out"][...]
        else:
            rows_sent[k - 1].wait_recv()
            row_grad = b["row_in"][k - 1]
        if k == 1:
            rows_sent.append(pass_on(b["row_in"].at[0], b["row_in"], "sr", "rr", 2, ahead))
        if k == 3:
            merged_sent = [
                send_seq(b["merged"].at[t], b["merged"].at[t], b["sm"].at[i], b["rm"].at[i], to)
                for i, to in enumerate((ahead, behind))
            ]
        rows = pl.ds(pl.multiple_of(source * share, share), share)
        attn = dims(row_grad, w_proj[...], 1, 1).astype(bf)
        queries = b["query"][rows, :]
        outs = []
        for h in range(heads):
            at = slice(h * HEAD, (h + 1) * HEAD)
            below = slice(local + h * HEAD, local + (h + 1) * HEAD)
            attn_h = attn[:, at]
            prob_grad = mm(attn_h, b["key_value"][below])
            probs = b["probs"][h, rows, :]
            value_grad = dims(attn_h, probs.astype(bf), 0, 0)
            inner = jnp.sum(prob_grad * probs, axis=-1, keepdims=True)
            score_grad = (probs * (prob_grad - inner) * scaling).astype(bf)
            outs.append(dims(score_grad, b["key_value"][at], 1, 1))
            key_grad = dims(queries[:, at], score_grad, 0, 0)
            if k == 0:
                b["kv_grad"][at] = key_grad
                b["kv_grad"][below] = value_grad
            else:
                b["kv_grad"][at] += key_grad
                b["kv_grad"][below] += value_grad
        b["query_grad"][rows, :] = jnp.concatenate(outs, axis=1).astype(bf)

    kv_grad = b["kv_grad"][...].astype(bf)

    def permuted(shift):
        hot = one_hot(first_rows(s), shift, s.rows)
        return (dims(hot[:, :local], b["query_grad"][...], 1, 1) + mm(hot[:, local:], kv_grad)).astype(bf)

    def relay():
        merged_sent[0].wait_recv()
        merged_sent.append(
            send_seq(b["merged"].at[behind], b["merged"].at[behind], b["sm"].at[2], b["rm"].at[2], ahead)
        )

    def between():
        for copy in merged_sent[1:]:
            copy.wait_recv()
        every = b["merged"][...].reshape(block, width)
        value = mm(select, every).astype(bf)
        for q in range(4):
            placed_ref[:, q * width : (q + 1) * width] = value[q * share : (q + 1) * share]

    clip_sum(s, place, permuted, shared, relay, between, summed_ref, b)
    for copies in (ups, parts, rows_sent, merged_sent):
        for copy in copies:
            copy.wait_send()


def fused(s, n, *operands):
    patches, w_proj = operands[1], operands[7]
    block, width = patches.shape
    local = w_proj.shape[0]
    scratch = block_scratch(block, width, local, n) | reduce_scratch(s, width, block)
    vmem = pl.BlockSpec(memory_space=pltpu.VMEM)
    anywhere = pl.BlockSpec(memory_space=pl.ANY)
    specs = [vmem] * len(operands)
    specs[0] = pl.BlockSpec(memory_space=pltpu.SMEM)
    for i in (1, 5, 7, 11):
        specs[i] = anywhere
    return pl.pallas_call(
        functools.partial(block_kernel, s, n, tuple(scratch)),
        out_shape=(
            pltpu.VMEM((block // n, 4 * width), jnp.bfloat16),
            jax.ShapeDtypeStruct((s.per, 1, width), jnp.float32),
        ),
        in_specs=specs,
        out_specs=(vmem,) * 2,
        scratch_shapes=list(scratch.values()),
        compiler_params=pltpu.CompilerParams(
            collective_id=0, has_side_effects=True, vmem_limit_bytes=60000 * 1024
        ),
    )(*operands)


def body(
    rows_y, rows_z, seq,
    patches, clip_tokens, positions, norm_gain, norm_bias, w_qkv, b_qkv, w_proj, b_proj,
    merge_gain, merge_bias, grad_placed,
):
    width = patches.shape[1]
    weights = w_qkv.transpose(1, 2, 0).reshape(-1, width)
    s = Sizes(rows_y, rows_z, width, weights.shape[0])
    placed, summed = fused(
        s, seq, clip_tokens, patches, positions, norm_gain, norm_bias, weights, b_qkv,
        w_proj, b_proj, merge_gain, merge_bias, grad_placed,
    )
    return placed, summed.transpose(1, 0, 2)


def build(mesh, rows_y, rows_z):
    placed = (
        P("clip", None), P("clip"), P("clip", None), P(), P(), P(None, None, "seq"),
        P(None, "seq"), P("seq", None), P(), P(), P(), P(("clip", "seq"), None),
    )
    return jax.shard_map(
        functools.partial(body, rows_y, rows_z, mesh.shape["seq"]),
        mesh=mesh,
        in_specs=placed,
        out_specs=(P(("clip", "seq"), None), P("seq", "clip", None)),
        check_vma=False,
    )


def solution(mesh):
    return build(mesh, 8, 12)
```

```python
import functools

import jax
import jax.numpy as jnp
import numpy as np
from jax import lax
from jax.experimental import pallas as pl
from jax.experimental.pallas import tpu as pltpu
from jax.sharding import PartitionSpec as P

HEAD = 80
MESH = pl.DeviceIdType.MESH
EPSILON = 1e-06


def one_hot(sources, shift, width):
    lanes = lax.broadcasted_iota(jnp.int32, (sources.shape[0], width), 1)
    return (lanes == sources + shift).astype(jnp.float32).astype(jnp.bfloat16)


def up_to(count, unit):
    return -(-count // unit) * unit


class Sizes:
    def __init__(self, rows_y, rows_z, width, rows):
        self.ny, self.nz = rows_y // 2, rows_z // 2
        self.rows = rows
        self.per = rows // (2 * rows_y * rows_z)
        self.ca = up_to(self.per * self.nz, 16)
        self.cb = up_to(self.per * self.ny, 8)
        self.wa = 6 * 128
        self.wb = width - self.wa
        self.ka, self.kb = self.wa // 128, self.wb // 128
        self.ra, self.rb = up_to(self.per * self.ka, 16), up_to(self.per * self.kb, 16)


def source_rows(groups, length, count, unit, steps):
    row = lax.broadcasted_iota(jnp.int32, (groups * length, 1), 0)
    group, inside = lax.div(row, length), lax.rem(row, length)
    major, minor = lax.div(inside, unit), lax.rem(inside, unit)
    source = group * steps[0] + major * steps[1] + minor
    return jnp.where(inside < count * unit, source, -100000)


def first_rows(s):
    return source_rows(s.ny, s.ca, s.nz, s.per, (8 * s.per * s.nz, 4 * s.per))


def second_rows(s):
    return source_rows(s.nz, s.cb, s.ny, s.per, (s.per, s.ca))


def third_rows(s):
    return source_rows(s.nz, s.ra, s.ka, s.per, (s.per, s.ca))


def fourth_rows(s):
    return source_rows(s.ny, s.rb, s.kb, s.per, (s.per, s.cb))


def tiles_down(values):
    return jnp.concatenate(
        [values[:, k : k + 128] for k in range(0, values.shape[1], 128)], axis=0
    )


def near_first(count):
    return sorted(range(1, count), key=lambda k: (min(k, count - k), k))


def send(source, target, send_sem, recv_sem, clip):
    copy = pltpu.make_async_remote_copy(
        src_ref=source, dst_ref=target, send_sem=send_sem, recv_sem=recv_sem,
        device_id={"clip": clip}, device_id_type=MESH,
    )
    copy.start()
    return copy


def reduce_scratch(s, width, block):
    bf = jnp.bfloat16
    dma = pltpu.SemaphoreType.DMA
    return dict(
        hot_q=pltpu.VMEM((8, s.ny * s.ca, s.rows // 3), bf),
        hot_kv=pltpu.VMEM((8, s.ny * s.ca, s.rows // 3 * 2), bf),
        give=pltpu.VMEM((8, s.ny * s.ca, block), bf),
        got=pltpu.VMEM((8, s.ny * s.ca, block), bf),
        others=pltpu.VMEM((8, block, width), bf),
        out_a=pltpu.VMEM((s.ny, s.ca, s.wa), bf),
        in_a=pltpu.VMEM((s.ny, s.ca, s.wa), bf),
        out_b=pltpu.VMEM((s.nz, s.cb, s.wb), bf),
        in_b=pltpu.VMEM((s.nz, s.cb, s.wb), bf),
        out_c=pltpu.VMEM((s.nz, s.ra, 128), bf),
        in_c=pltpu.VMEM((s.nz, s.ra, 128), bf),
        out_d=pltpu.VMEM((s.ny, s.rb, 128), bf),
        in_d=pltpu.VMEM((s.ny, s.rb, 128), bf),
        sn=dma((8,)), rn=dma((8,)),
        sp=dma((8,)), rp=dma((8,)),
        sa=dma((s.ny,)), ra=dma((s.ny,)),
        sb=dma((s.nz,)), rb=dma((s.nz,)),
        sc=dma((s.nz,)), rc=dma((s.nz,)),
        sd=dma((s.ny,)), rd=dma((s.ny,)),
    )


def place_of(s):
    me = lax.axis_index("clip")
    core = lax.rem(me, 2)
    chip = lax.div(me, 2)
    z = lax.rem(chip, 2 * s.nz)
    y = lax.div(chip, 2 * s.nz)
    return lax.div(y, 2), lax.div(z, 2), lax.rem(y, 2), lax.rem(z, 2), core


def clip_of(s, place):
    y, z, odd_y, odd_z, core = place
    return ((2 * y + odd_y) * 2 * s.nz + 2 * z + odd_z) * 2 + core


def flipped(place, k):
    y, z, *bits = place
    return (y, z, *(1 - bit if k & (4 >> i) else bit for i, bit in enumerate(bits)))


def along_y(place, count, k):
    return (lax.rem(place[0] + k, count),) + place[1:]


def along_z(place, count, k):
    return (place[0], lax.rem(place[1] + k, count)) + place[2:]


def greet(s, place):
    barrier = pltpu.get_barrier_semaphore()
    others = [flipped(place, k) for k in range(1, 8)]
    others += [along_y(place, s.ny, k) for k in range(1, s.ny)]
    others += [along_z(place, s.nz, k) for k in range(1, s.nz)]
    for other in others:
        pl.semaphore_signal(
            barrier, inc=1, device_id={"clip": clip_of(s, other)}, device_id_type=MESH
        )
    return len(others)


def mm(left, right):
    return jnp.dot(left, right, preferred_element_type=jnp.float32)


def spread(s, out, arrived, send_sem, recv_sem, place, dim):
    along, count = ((along_y, s.ny), (along_z, s.nz))[dim]
    copies = []
    for k in near_first(count):
        other = along(place, count, k)
        copies.append((k, send(
            out.at[other[dim]], arrived.at[k], send_sem.at[k], recv_sem.at[k], clip_of(s, other)
        )))
    return copies


def added(out, arrived, copies, mine):
    total = out[mine].astype(jnp.float32)
    for k, copy in copies:
        copy.wait_recv()
        total = total + arrived[k].astype(jnp.float32)
    return total


def share_normed(s, place, b):
    copies = {}
    for k in (6, 4, 2, 1):
        copies[k] = send(
            b["normed"], b["others"].at[k], b["sn"].at[k], b["rn"].at[k], clip_of(s, flipped(place, k))
        )
    return copies


def clip_sum(s, place, permuted, normed, relay, between, summed_ref, b):
    y, z = place[:2]
    bf = jnp.bfloat16

    given = {}
    for k in (6, 7, 4, 5, 2, 3, 1):
        other = flipped(place, k)
        b["give"][k] = permuted(k)
        given[k] = send(b["give"].at[k], b["got"].at[k], b["sp"].at[k], b["rp"].at[k], clip_of(s, other))
    pair = clip_of(s, flipped(place, 1))
    for k in (2, 4, 6):
        normed[k].wait_recv()
        normed[k + 1] = send(
            b["others"].at[k], b["others"].at[k + 1], b["sn"].at[k + 1], b["rn"].at[k + 1], pair
        )
    value = mm(permuted(0), b["normed"][...])
    relay()
    for k in (1, 2, 4, 3, 5, 6, 7):
        if k & 1:
            normed[k].wait_recv()
        given[k].wait_recv()
        value = value + mm(b["got"][k], b["others"][k])
    b["out_a"][...] = value[:, : s.wa].reshape(s.ny, s.ca, s.wa).astype(bf)
    copies_a = spread(s, b["out_a"], b["in_a"], b["sa"], b["ra"], place, 0)
    value = mm(one_hot(second_rows(s), 0, s.ny * s.ca), value[:, s.wa :].astype(bf))
    b["out_b"][...] = value.reshape(s.nz, s.cb, s.wb).astype(bf)
    copies_b = spread(s, b["out_b"], b["in_b"], b["sb"], b["rb"], place, 1)
    between()
    total = tiles_down(added(b["out_a"], b["in_a"], copies_a, y)).astype(bf)
    value = mm(one_hot(third_rows(s), 0, s.ka * s.ca), total)
    b["out_c"][...] = value.reshape(s.nz, s.ra, 128).astype(bf)
    copies_c = spread(s, b["out_c"], b["in_c"], b["sc"], b["rc"], place, 1)
    total = tiles_down(added(b["out_b"], b["in_b"], copies_b, z)).astype(bf)
    value = mm(one_hot(fourth_rows(s), 0, s.kb * s.cb), total)
    b["out_d"][...] = value.reshape(s.ny, s.rb, 128).astype(bf)
    copies_d = spread(s, b["out_d"], b["in_d"], b["sd"], b["rd"], place, 0)
    total = added(b["out_c"], b["in_c"], copies_c, z)
    for k in range(s.ka):
        summed_ref[:, 0, k * 128 : (k + 1) * 128] = total[k * s.per : (k + 1) * s.per]
    total = added(b["out_d"], b["in_d"], copies_d, y)
    for k in range(s.kb):
        summed_ref[:, 0, s.wa + k * 128 : s.wa + (k + 1) * 128] = total[k * s.per : (k + 1) * s.per]
    for copies in (normed, given):
        for copy in copies.values():
            copy.wait_send()
    for copies in (copies_a, copies_b, copies_c, copies_d):
        for _, copy in copies:
            copy.wait_send()


def normalize(values, gain_row, bias_row):
    center = values - jnp.mean(values, axis=-1, keepdims=True)
    inverse = lax.rsqrt(jnp.mean(center * center, axis=-1, keepdims=True) + EPSILON)
    unit_rows = center * inverse
    return (unit_rows * gain_row + bias_row, unit_rows, inverse)


def normalize_back(upstream, unit_rows, inverse, gain_row):
    scaled = upstream * gain_row
    return inverse * (
        scaled
        - jnp.mean(scaled, axis=-1, keepdims=True)
        - unit_rows * jnp.mean(scaled * unit_rows, axis=-1, keepdims=True)
    )


def vector(ref):
    return ref[...].reshape(1, ref.shape[0])


def dims(left, right, a, b):
    return lax.dot_general(
        left, right, (((a,), (b,)), ((), ())), preferred_element_type=jnp.float32
    )


def send_seq(source, target, send_sem, recv_sem, seq):
    copy = pltpu.make_async_remote_copy(
        src_ref=source, dst_ref=target, send_sem=send_sem, recv_sem=recv_sem,
        device_id={"seq": seq}, device_id_type=MESH,
    )
    copy.start()
    return copy


def block_scratch(block, width, local, n):
    bf, f32 = jnp.bfloat16, jnp.float32
    dma = pltpu.SemaphoreType.DMA
    share = block // n
    return dict(
        normed=pltpu.VMEM((block, width), bf),
        query=pltpu.VMEM((block, local), bf),
        key_value=pltpu.VMEM((2 * local, block), bf),
        probs=pltpu.VMEM((local // HEAD, block, block), f32),
        biases=pltpu.VMEM((8, 384), f32),
        up_out=pltpu.VMEM((n, share, width), bf),
        up_in=pltpu.VMEM((3, share, width), bf),
        part_out=pltpu.VMEM((3, share, width), bf),
        part_in=pltpu.VMEM((3, share, width), bf),
        row_out=pltpu.VMEM((share, width), bf),
        row_in=pltpu.VMEM((3, share, width), bf),
        loads=dma((len(ORDER),)),
        merged=pltpu.VMEM((n, share, width), bf),
        query_grad=pltpu.VMEM((block, local), bf),
        kv_grad=pltpu.VMEM((2 * local, block), f32),
        su=dma((3,)), ru=dma((3,)),
        sq=dma((3,)), rq=dma((3,)),
        sr=dma((3,)), rr=dma((3,)),
        sm=dma((3,)), rm=dma((3,)),
    )


ORDER = (
    "tokens", "positions", "grads", "norm_gain", "norm_bias", "patches", "weights", "b_qkv",
    "w_proj", "b_proj", "merge_gain", "merge_bias",
)


def block_kernel(s, n, names, *refs):
    operands = tuple(zip(ORDER, refs[: len(ORDER)]))
    placed_ref, summed_ref, *scratch = refs[len(ORDER) :]
    b = dict(zip(names, scratch))
    loads = {}
    for i, (name, source) in enumerate(operands):
        loads[name] = pltpu.make_async_copy(source, b["in_" + name], b["loads"].at[i])
        loads[name].start()

    def loaded(name):
        loads[name].wait()
        return b["in_" + name]

    bf, f32, i32 = jnp.bfloat16, jnp.float32, jnp.int32
    patches, w_proj = b["in_patches"], b["in_w_proj"]
    block, width = patches.shape
    local = w_proj.shape[0]
    heads = local // HEAD
    share = block // n
    scaling = HEAD ** (-0.5)
    place = place_of(s)
    core = place[4]
    t = lax.axis_index("seq")
    ahead = lax.rem(t + 1 + 2 * core, n)
    behind = lax.rem(t + 3 - 2 * core, n)
    across = lax.rem(t + 2, n)
    partners = greet(s, place)
    for k in range(1, n):
        pl.semaphore_signal(
            pltpu.get_barrier_semaphore(), inc=1,
            device_id={"seq": lax.rem(t + k, n)}, device_id_type=MESH,
        )
    live = loaded("tokens")[0]

    spread_out = lax.broadcasted_iota(i32, (block // 4, block), 1)
    token_of = lax.broadcasted_iota(i32, (block // 4, block), 0)
    spread_out = ((spread_out >> 2) == token_of).astype(f32).astype(bf)
    places = jnp.broadcast_to(loaded("positions")[...].astype(f32), (8, block // 4)).astype(bf)
    places = mm(places, spread_out)[0:1].astype(i32)
    slot = lax.broadcasted_iota(i32, (1, block), 1)
    code = jnp.where(slot < 4 * live, places * 4 + (slot & 3), -1)
    row = lax.broadcasted_iota(i32, (4 * share, block), 0)
    wanted = (t * share + lax.rem(row, share)) * 4 + lax.div(row, share)
    select = (code == wanted).astype(f32).astype(bf)
    grads = loaded("grads")
    stacked = jnp.concatenate([grads[:, q * width : (q + 1) * width] for q in range(4)], axis=0)
    b["up_out"][...] = dims(select, stacked, 0, 0).reshape(n, share, width).astype(bf)
    pl.semaphore_wait(pltpu.get_barrier_semaphore(), partners + n - 1)
    def pass_on(out, arrived, sends, arrivals, i, to):
        return send_seq(out, arrived.at[i], b[sends].at[i], b[arrivals].at[i], to)

    ups = [
        pass_on(b["up_out"].at[across], b["up_in"], "su", "ru", 0, ahead),
        pass_on(b["up_out"].at[behind], b["up_in"], "su", "ru", 1, behind),
    ]
    norm_gain, norm_bias = loaded("norm_gain"), loaded("norm_bias")
    loaded("patches")
    b["normed"][...] = normalize(patches[...].astype(f32), vector(norm_gain), vector(norm_bias))[0].astype(bf)
    shared = share_normed(s, place, b)
    weights, b_qkv = loaded("weights"), loaded("b_qkv")
    normed = b["normed"][...]
    b["query"][...] = (dims(normed, weights[:local], 1, 1) + b_qkv[0:1]).astype(bf)
    b["biases"][...] = jnp.zeros((8, 384), f32)
    b["biases"][0:2, :local] = b_qkv[1:3]
    columns = b["biases"][...].T
    for p in (0, 1):
        value = dims(weights[(1 + p) * local : (2 + p) * local], normed, 1, 1)
        b["key_value"][p * local : (p + 1) * local] = (value + columns[:local, p : p + 1]).astype(bf)

    live_keys = lax.broadcasted_iota(i32, (share, block), 1) < 4 * live
    loaded("w_proj")
    parts = []

    def attend(to):
        rows = pl.ds(pl.multiple_of(to * share, share), share)
        queries = b["query"][rows, :]
        outs = []
        for h in range(heads):
            at = slice(h * HEAD, (h + 1) * HEAD)
            scores = mm(queries[:, at], b["key_value"][at]) * scaling
            scores = jnp.where(live_keys, scores, -1e30)
            powers = jnp.exp(scores - jnp.max(scores, axis=-1, keepdims=True))
            probs = powers * (1.0 / jnp.sum(powers, axis=-1, keepdims=True))
            b["probs"][h, rows, :] = probs
            outs.append(dims(probs.astype(bf), b["key_value"][local + h * HEAD : local + (h + 1) * HEAD], 1, 1))
        attended = jnp.concatenate(outs, axis=1).astype(bf)
        return mm(attended, w_proj[...])

    b["part_out"][0] = attend(across).astype(bf)
    parts.append(pass_on(b["part_out"].at[0], b["part_in"], "sq", "rq", 0, ahead))
    b["part_out"][1] = attend(behind).astype(bf)
    parts.append(pass_on(b["part_out"].at[1], b["part_in"], "sq", "rq", 1, behind))
    ups[0].wait_recv()
    b["up_out"][ahead] = (b["up_out"][ahead].astype(f32) + b["up_in"][0].astype(f32)).astype(bf)
    ups.append(pass_on(b["up_out"].at[ahead], b["up_in"], "su", "ru", 2, ahead))
    part = attend(ahead)
    parts[0].wait_recv()
    b["part_out"][2] = (part + b["part_in"][0].astype(f32)).astype(bf)
    parts.append(pass_on(b["part_out"].at[2], b["part_in"], "sq", "rq", 2, ahead))
    own = pl.ds(pl.multiple_of(t * share, share), share)
    output = attend(t)
    for k in range(8):
        other = flipped(place, k)
        shift = ((other[2] * 2 * s.nz + other[3]) * 2 + other[4]) * s.per
        b["hot_q"][k] = one_hot(first_rows(s), shift, local)
        b["hot_kv"][k] = one_hot(first_rows(s), shift - local, 2 * local)
    b_proj, merge_gain, merge_bias = (loaded(name) for name in ("b_proj", "merge_gain", "merge_bias"))
    output = output + vector(b_proj) + patches[own, :].astype(f32)
    upstream = b["up_out"][t].astype(f32)
    for i in (1, 2):
        ups[i].wait_recv()
        upstream = upstream + b["up_in"][i].astype(f32)
    for i in (1, 2):
        parts[i].wait_recv()
        output = output + b["part_in"][i].astype(f32)
    merged, unit_rows, inverse = normalize(output, vector(merge_gain), vector(merge_bias))
    b["row_out"][...] = normalize_back(upstream, unit_rows, inverse, vector(merge_gain)).astype(bf)
    rows_sent = [
        pass_on(b["row_out"], b["row_in"], "sr", "rr", 0, ahead),
        pass_on(b["row_out"], b["row_in"], "sr", "rr", 1, behind),
    ]
    b["merged"][t] = merged.astype(bf)

    for k, source in enumerate((t, behind, ahead, across)):
        if k == 0:
            row_grad = b["row_out"][...]
        else:
            rows_sent[k - 1].wait_recv()
            row_grad = b["row_in"][k - 1]
        if k == 1:
            rows_sent.append(pass_on(b["row_in"].at[0], b["row_in"], "sr", "rr", 2, ahead))
        if k == 3:
            merged_sent = [
                send_seq(b["merged"].at[t], b["merged"].at[t], b["sm"].at[i], b["rm"].at[i], to)
                for i, to in enumerate((ahead, behind))
            ]
        rows = pl.ds(pl.multiple_of(source * share, share), share)
        attn = dims(row_grad, w_proj[...], 1, 1).astype(bf)
        queries = b["query"][rows, :]
        outs = []
        for h in range(heads):
            at = slice(h * HEAD, (h + 1) * HEAD)
            below = slice(local + h * HEAD, local + (h + 1) * HEAD)
            attn_h = attn[:, at]
            prob_grad = mm(attn_h, b["key_value"][below])
            probs = b["probs"][h, rows, :]
            value_grad = dims(attn_h, probs.astype(bf), 0, 0)
            inner = jnp.sum(prob_grad * probs, axis=-1, keepdims=True)
            score_grad = (probs * (prob_grad - inner) * scaling).astype(bf)
            outs.append(dims(score_grad, b["key_value"][at], 1, 1))
            key_grad = dims(queries[:, at], score_grad, 0, 0)
            if k == 0:
                b["kv_grad"][at] = key_grad
                b["kv_grad"][below] = value_grad
            else:
                b["kv_grad"][at] += key_grad
                b["kv_grad"][below] += value_grad
        b["query_grad"][rows, :] = jnp.concatenate(outs, axis=1).astype(bf)

    kv_grad = b["kv_grad"][...].astype(bf)

    def permuted(k):
        value = dims(b["hot_q"][k], b["query_grad"][...], 1, 1) + mm(b["hot_kv"][k], kv_grad)
        return value.astype(bf)

    def relay():
        merged_sent[0].wait_recv()
        merged_sent.append(
            send_seq(b["merged"].at[behind], b["merged"].at[behind], b["sm"].at[2], b["rm"].at[2], ahead)
        )

    def between():
        for copy in merged_sent[1:]:
            copy.wait_recv()
        every = b["merged"][...].reshape(block, width)
        value = mm(select, every).astype(bf)
        for q in range(4):
            placed_ref[:, q * width : (q + 1) * width] = value[q * share : (q + 1) * share]

    clip_sum(s, place, permuted, shared, relay, between, summed_ref, b)
    for copies in (ups, parts, rows_sent, merged_sent):
        for copy in copies:
            copy.wait_send()


def fused(s, n, **operands):
    block, width = operands["patches"].shape
    local = operands["w_proj"].shape[0]
    scratch = block_scratch(block, width, local, n) | reduce_scratch(s, width, block)
    for name in ORDER:
        space = pltpu.SMEM if name == "tokens" else pltpu.VMEM
        scratch["in_" + name] = space(operands[name].shape, operands[name].dtype)
    vmem = pl.BlockSpec(memory_space=pltpu.VMEM)
    return pl.pallas_call(
        functools.partial(block_kernel, s, n, tuple(scratch)),
        out_shape=(
            pltpu.VMEM((block // n, 4 * width), jnp.bfloat16),
            pltpu.VMEM((s.per, 1, width), jnp.float32),
        ),
        in_specs=[pl.BlockSpec(memory_space=pl.ANY)] * len(ORDER),
        out_specs=(vmem,) * 2,
        scratch_shapes=list(scratch.values()),
        compiler_params=pltpu.CompilerParams(
            collective_id=0, has_side_effects=True, vmem_limit_bytes=60000 * 1024
        ),
    )(*(operands[name] for name in ORDER))


def body(
    rows_y, rows_z, seq,
    patches, clip_tokens, positions, norm_gain, norm_bias, w_qkv, b_qkv, w_proj, b_proj,
    merge_gain, merge_bias, grad_placed,
):
    width = patches.shape[1]
    weights = w_qkv.transpose(1, 2, 0).reshape(-1, width)
    s = Sizes(rows_y, rows_z, width, weights.shape[0])
    placed, summed = fused(
        s, seq, tokens=clip_tokens, patches=patches, positions=positions, norm_gain=norm_gain,
        norm_bias=norm_bias, weights=weights, b_qkv=b_qkv, w_proj=w_proj, b_proj=b_proj,
        merge_gain=merge_gain, merge_bias=merge_bias, grads=grad_placed,
    )
    return placed, summed.transpose(1, 0, 2)


def build(mesh, rows_y, rows_z):
    placed = (
        P("clip", None), P("clip"), P("clip", None), P(), P(), P(None, None, "seq"),
        P(None, "seq"), P("seq", None), P(), P(), P(), P(("clip", "seq"), None),
    )
    return jax.shard_map(
        functools.partial(body, rows_y, rows_z, mesh.shape["seq"]),
        mesh=mesh,
        in_specs=placed,
        out_specs=(P(("clip", "seq"), None), P("seq", "clip", None)),
        check_vma=False,
    )


def solution(mesh):
    return build(mesh, 8, 12)
```

```python
import functools

import jax
import jax.numpy as jnp
import numpy as np
from jax import lax
from jax.experimental import pallas as pl
from jax.experimental.pallas import tpu as pltpu
from jax.sharding import PartitionSpec as P

HEAD = 80
MESH = pl.DeviceIdType.MESH
EPSILON = 1e-06


def one_hot(sources, shift, width):
    lanes = lax.broadcasted_iota(jnp.int32, (sources.shape[0], width), 1)
    return (lanes == sources + shift).astype(jnp.float32).astype(jnp.bfloat16)


def up_to(count, unit):
    return -(-count // unit) * unit


class Sizes:
    def __init__(self, rows_y, rows_z, width, rows):
        self.ny, self.nz = rows_y // 2, rows_z // 2
        self.rows = rows
        self.per = rows // (2 * rows_y * rows_z)
        self.ca = up_to(self.per * self.nz, 16)
        self.cb = up_to(self.per * self.ny, 8)
        self.wa = 6 * 128
        self.wb = width - self.wa
        self.ka, self.kb = self.wa // 128, self.wb // 128
        self.ra, self.rb = up_to(self.per * self.ka, 16), up_to(self.per * self.kb, 16)


def source_rows(groups, length, count, unit, steps):
    row = lax.broadcasted_iota(jnp.int32, (groups * length, 1), 0)
    group, inside = lax.div(row, length), lax.rem(row, length)
    major, minor = lax.div(inside, unit), lax.rem(inside, unit)
    source = group * steps[0] + major * steps[1] + minor
    return jnp.where(inside < count * unit, source, -100000)


def first_rows(s):
    return source_rows(s.ny, s.ca, s.nz, s.per, (8 * s.per * s.nz, 4 * s.per))


def second_rows(s):
    return source_rows(s.nz, s.cb, s.ny, s.per, (s.per, s.ca))


def third_rows(s):
    return source_rows(s.nz, s.ra, s.ka, s.per, (s.per, s.ca))


def fourth_rows(s):
    return source_rows(s.ny, s.rb, s.kb, s.per, (s.per, s.cb))


def tiles_down(values):
    return jnp.concatenate(
        [values[:, k : k + 128] for k in range(0, values.shape[1], 128)], axis=0
    )


def far_first(count):
    return sorted(range(1, count), key=lambda k: (-min(k, count - k), k))


def send(source, target, send_sem, recv_sem, clip):
    copy = pltpu.make_async_remote_copy(
        src_ref=source, dst_ref=target, send_sem=send_sem, recv_sem=recv_sem,
        device_id={"clip": clip}, device_id_type=MESH,
    )
    copy.start()
    return copy


def reduce_scratch(s, width, block):
    bf = jnp.bfloat16
    dma = pltpu.SemaphoreType.DMA
    return dict(
        hot_q=pltpu.VMEM((8, s.ny * s.ca, s.rows // 3), bf),
        hot_kv=pltpu.VMEM((8, s.ny * s.ca, s.rows // 3 * 2), bf),
        give=pltpu.VMEM((8, s.ny * s.ca, block), bf),
        got=pltpu.VMEM((8, s.ny * s.ca, block), bf),
        others=pltpu.VMEM((8, block, width), bf),
        out_a=pltpu.VMEM((s.ny, s.ca, s.wa), bf),
        in_a=pltpu.VMEM((s.ny, s.ca, s.wa), bf),
        out_b=pltpu.VMEM((s.nz, s.cb, s.wb), bf),
        in_b=pltpu.VMEM((s.nz, s.cb, s.wb), bf),
        out_c=pltpu.VMEM((s.nz, s.ra, 128), bf),
        in_c=pltpu.VMEM((s.nz, s.ra, 128), bf),
        out_d=pltpu.VMEM((s.ny, s.rb, 128), bf),
        in_d=pltpu.VMEM((s.ny, s.rb, 128), bf),
        sn=dma((8,)), rn=dma((8,)),
        sp=dma((8,)), rp=dma((8,)),
        sa=dma((s.ny,)), ra=dma((s.ny,)),
        sb=dma((s.nz,)), rb=dma((s.nz,)),
        sc=dma((s.nz,)), rc=dma((s.nz,)),
        sd=dma((s.ny,)), rd=dma((s.ny,)),
    )


def place_of(s):
    me = lax.axis_index("clip")
    core = lax.rem(me, 2)
    chip = lax.div(me, 2)
    z = lax.rem(chip, 2 * s.nz)
    y = lax.div(chip, 2 * s.nz)
    return lax.div(y, 2), lax.div(z, 2), lax.rem(y, 2), lax.rem(z, 2), core


def clip_of(s, place):
    y, z, odd_y, odd_z, core = place
    return ((2 * y + odd_y) * 2 * s.nz + 2 * z + odd_z) * 2 + core


def flipped(place, k):
    y, z, *bits = place
    return (y, z, *(1 - bit if k & (4 >> i) else bit for i, bit in enumerate(bits)))


def along_y(place, count, k):
    return (lax.rem(place[0] + k, count),) + place[1:]


def along_z(place, count, k):
    return (place[0], lax.rem(place[1] + k, count)) + place[2:]


def greet(s, place):
    barrier = pltpu.get_barrier_semaphore()
    others = [flipped(place, k) for k in range(1, 8)]
    others += [along_y(place, s.ny, k) for k in range(1, s.ny)]
    others += [along_z(place, s.nz, k) for k in range(1, s.nz)]
    for other in others:
        pl.semaphore_signal(
            barrier, inc=1, device_id={"clip": clip_of(s, other)}, device_id_type=MESH
        )
    return len(others)


def mm(left, right):
    return jnp.dot(left, right, preferred_element_type=jnp.float32)


def spread(s, out, arrived, send_sem, recv_sem, place, dim):
    along, count = ((along_y, s.ny), (along_z, s.nz))[dim]
    copies = []
    for k in far_first(count):
        other = along(place, count, k)
        copies.append((k, send(
            out.at[other[dim]], arrived.at[k], send_sem.at[k], recv_sem.at[k], clip_of(s, other)
        )))
    return copies


def added(out, arrived, copies, mine):
    total = out[mine].astype(jnp.float32)
    for k, copy in copies:
        copy.wait_recv()
        total = total + arrived[k].astype(jnp.float32)
    return total


def share_normed(s, place, b):
    copies = {}
    for k in (6, 4, 2, 1):
        copies[k] = send(
            b["normed"], b["others"].at[k], b["sn"].at[k], b["rn"].at[k], clip_of(s, flipped(place, k))
        )
    return copies


def clip_sum(s, place, permuted, normed, relay, between, summed_ref, b):
    y, z = place[:2]
    bf = jnp.bfloat16

    given = {}
    for k in (6, 7, 4, 5, 2, 3, 1):
        other = flipped(place, k)
        b["give"][k] = permuted(k)
        given[k] = send(b["give"].at[k], b["got"].at[k], b["sp"].at[k], b["rp"].at[k], clip_of(s, other))
    pair = clip_of(s, flipped(place, 1))
    for k in (2, 4, 6):
        normed[k].wait_recv()
        normed[k + 1] = send(
            b["others"].at[k], b["others"].at[k + 1], b["sn"].at[k + 1], b["rn"].at[k + 1], pair
        )
    value = mm(permuted(0), b["normed"][...])
    relay()
    for k in (1, 2, 4, 3, 5, 6, 7):
        if k & 1:
            normed[k].wait_recv()
        given[k].wait_recv()
        value = value + mm(b["got"][k], b["others"][k])
    b["out_a"][...] = value[:, : s.wa].reshape(s.ny, s.ca, s.wa).astype(bf)
    copies_a = spread(s, b["out_a"], b["in_a"], b["sa"], b["ra"], place, 0)
    value = mm(one_hot(second_rows(s), 0, s.ny * s.ca), value[:, s.wa :].astype(bf))
    b["out_b"][...] = value.reshape(s.nz, s.cb, s.wb).astype(bf)
    copies_b = spread(s, b["out_b"], b["in_b"], b["sb"], b["rb"], place, 1)
    between()
    total = tiles_down(added(b["out_a"], b["in_a"], copies_a, y)).astype(bf)
    value = mm(one_hot(third_rows(s), 0, s.ka * s.ca), total)
    b["out_c"][...] = value.reshape(s.nz, s.ra, 128).astype(bf)
    copies_c = spread(s, b["out_c"], b["in_c"], b["sc"], b["rc"], place, 1)
    total = tiles_down(added(b["out_b"], b["in_b"], copies_b, z)).astype(bf)
    value = mm(one_hot(fourth_rows(s), 0, s.kb * s.cb), total)
    b["out_d"][...] = value.reshape(s.ny, s.rb, 128).astype(bf)
    copies_d = spread(s, b["out_d"], b["in_d"], b["sd"], b["rd"], place, 0)
    total = added(b["out_c"], b["in_c"], copies_c, z)
    for k in range(s.ka):
        summed_ref[:, 0, k * 128 : (k + 1) * 128] = total[k * s.per : (k + 1) * s.per]
    total = added(b["out_d"], b["in_d"], copies_d, y)
    for k in range(s.kb):
        summed_ref[:, 0, s.wa + k * 128 : s.wa + (k + 1) * 128] = total[k * s.per : (k + 1) * s.per]
    for copies in (normed, given):
        for copy in copies.values():
            copy.wait_send()
    for copies in (copies_a, copies_b, copies_c, copies_d):
        for _, copy in copies:
            copy.wait_send()


def normalize(values, gain_row, bias_row):
    center = values - jnp.mean(values, axis=-1, keepdims=True)
    inverse = lax.rsqrt(jnp.mean(center * center, axis=-1, keepdims=True) + EPSILON)
    unit_rows = center * inverse
    return (unit_rows * gain_row + bias_row, unit_rows, inverse)


def normalize_back(upstream, unit_rows, inverse, gain_row):
    scaled = upstream * gain_row
    return inverse * (
        scaled
        - jnp.mean(scaled, axis=-1, keepdims=True)
        - unit_rows * jnp.mean(scaled * unit_rows, axis=-1, keepdims=True)
    )


def vector(ref):
    return ref[...].reshape(1, ref.shape[0])


def dims(left, right, a, b):
    return lax.dot_general(
        left, right, (((a,), (b,)), ((), ())), preferred_element_type=jnp.float32
    )


def send_seq(source, target, send_sem, recv_sem, seq):
    copy = pltpu.make_async_remote_copy(
        src_ref=source, dst_ref=target, send_sem=send_sem, recv_sem=recv_sem,
        device_id={"seq": seq}, device_id_type=MESH,
    )
    copy.start()
    return copy


def block_scratch(block, width, local, n):
    bf, f32 = jnp.bfloat16, jnp.float32
    dma = pltpu.SemaphoreType.DMA
    share = block // n
    return dict(
        normed=pltpu.VMEM((block, width), bf),
        query=pltpu.VMEM((block, local), bf),
        key_value=pltpu.VMEM((2 * local, block), bf),
        probs=pltpu.VMEM((local // HEAD, block, block), f32),
        biases=pltpu.VMEM((8, 384), f32),
        up_out=pltpu.VMEM((n, share, width), bf),
        up_in=pltpu.VMEM((3, share, width), bf),
        part_out=pltpu.VMEM((3, share, width), bf),
        part_in=pltpu.VMEM((3, share, width), bf),
        row_out=pltpu.VMEM((share, width), bf),
        row_in=pltpu.VMEM((3, share, width), bf),
        loads=dma((len(ORDER),)),
        merged=pltpu.VMEM((n, share, width), bf),
        query_grad=pltpu.VMEM((block, local), bf),
        kv_grad=pltpu.VMEM((2 * local, block), f32),
        su=dma((3,)), ru=dma((3,)),
        sq=dma((3,)), rq=dma((3,)),
        sr=dma((6,)), rr=dma((6,)),
        sm=dma((3,)), rm=dma((3,)),
    )


ORDER = (
    "tokens", "positions", "grads", "norm_gain", "norm_bias", "patches", "weights", "b_qkv",
    "w_proj", "b_proj", "merge_gain", "merge_bias",
)


def block_kernel(s, n, names, *refs):
    operands = tuple(zip(ORDER, refs[: len(ORDER)]))
    placed_ref, summed_ref, *scratch = refs[len(ORDER) :]
    b = dict(zip(names, scratch))
    loads = {}
    for i, (name, source) in enumerate(operands):
        loads[name] = pltpu.make_async_copy(source, b["in_" + name], b["loads"].at[i])
        loads[name].start()

    def loaded(name):
        loads[name].wait()
        return b["in_" + name]

    bf, f32, i32 = jnp.bfloat16, jnp.float32, jnp.int32
    patches, w_proj = b["in_patches"], b["in_w_proj"]
    block, width = patches.shape
    local = w_proj.shape[0]
    heads = local // HEAD
    share = block // n
    scaling = HEAD ** (-0.5)
    place = place_of(s)
    core = place[4]
    t = lax.axis_index("seq")
    ahead = lax.rem(t + 1 + 2 * core, n)
    behind = lax.rem(t + 3 - 2 * core, n)
    across = lax.rem(t + 2, n)
    partners = greet(s, place)
    for k in range(1, n):
        pl.semaphore_signal(
            pltpu.get_barrier_semaphore(), inc=1,
            device_id={"seq": lax.rem(t + k, n)}, device_id_type=MESH,
        )
    live = loaded("tokens")[0]

    spread_out = lax.broadcasted_iota(i32, (block // 4, block), 1)
    token_of = lax.broadcasted_iota(i32, (block // 4, block), 0)
    spread_out = ((spread_out >> 2) == token_of).astype(f32).astype(bf)
    places = jnp.broadcast_to(loaded("positions")[...].astype(f32), (8, block // 4)).astype(bf)
    places = mm(places, spread_out)[0:1].astype(i32)
    slot = lax.broadcasted_iota(i32, (1, block), 1)
    code = jnp.where(slot < 4 * live, places * 4 + (slot & 3), -1)
    row = lax.broadcasted_iota(i32, (4 * share, block), 0)
    wanted = (t * share + lax.rem(row, share)) * 4 + lax.div(row, share)
    select = (code == wanted).astype(f32).astype(bf)
    grads = loaded("grads")
    stacked = jnp.concatenate([grads[:, q * width : (q + 1) * width] for q in range(4)], axis=0)
    b["up_out"][...] = dims(select, stacked, 0, 0).reshape(n, share, width).astype(bf)
    pl.semaphore_wait(pltpu.get_barrier_semaphore(), partners + n - 1)
    def pass_on(out, arrived, sends, arrivals, i, to):
        return send_seq(out, arrived.at[i], b[sends].at[i], b[arrivals].at[i], to)

    ups = [
        pass_on(b["up_out"].at[across], b["up_in"], "su", "ru", 0, ahead),
        pass_on(b["up_out"].at[behind], b["up_in"], "su", "ru", 1, behind),
    ]
    norm_gain, norm_bias = loaded("norm_gain"), loaded("norm_bias")
    loaded("patches")
    b["normed"][...] = normalize(patches[...].astype(f32), vector(norm_gain), vector(norm_bias))[0].astype(bf)
    shared = share_normed(s, place, b)
    weights, b_qkv = loaded("weights"), loaded("b_qkv")
    normed = b["normed"][...]
    b["query"][...] = (dims(normed, weights[:local], 1, 1) + b_qkv[0:1]).astype(bf)
    b["biases"][...] = jnp.zeros((8, 384), f32)
    b["biases"][0:2, :local] = b_qkv[1:3]
    columns = b["biases"][...].T
    for p in (0, 1):
        value = dims(weights[(1 + p) * local : (2 + p) * local], normed, 1, 1)
        b["key_value"][p * local : (p + 1) * local] = (value + columns[:local, p : p + 1]).astype(bf)

    live_keys = lax.broadcasted_iota(i32, (share, block), 1) < 4 * live
    loaded("w_proj")
    parts = []

    def attend(to):
        rows = pl.ds(pl.multiple_of(to * share, share), share)
        queries = b["query"][rows, :]
        outs = []
        for h in range(heads):
            at = slice(h * HEAD, (h + 1) * HEAD)
            scores = mm(queries[:, at], b["key_value"][at]) * scaling
            scores = jnp.where(live_keys, scores, -1e30)
            powers = jnp.exp(scores - jnp.max(scores, axis=-1, keepdims=True))
            probs = powers * (1.0 / jnp.sum(powers, axis=-1, keepdims=True))
            b["probs"][h, rows, :] = probs
            outs.append(dims(probs.astype(bf), b["key_value"][local + h * HEAD : local + (h + 1) * HEAD], 1, 1))
        attended = jnp.concatenate(outs, axis=1).astype(bf)
        return mm(attended, w_proj[...])

    b["part_out"][0] = attend(across).astype(bf)
    parts.append(pass_on(b["part_out"].at[0], b["part_in"], "sq", "rq", 0, ahead))
    b["part_out"][1] = attend(behind).astype(bf)
    parts.append(pass_on(b["part_out"].at[1], b["part_in"], "sq", "rq", 1, behind))
    ups[0].wait_recv()
    b["up_out"][ahead] = (b["up_out"][ahead].astype(f32) + b["up_in"][0].astype(f32)).astype(bf)
    ups.append(pass_on(b["up_out"].at[ahead], b["up_in"], "su", "ru", 2, ahead))
    part = attend(ahead)
    parts[0].wait_recv()
    b["part_out"][2] = (part + b["part_in"][0].astype(f32)).astype(bf)
    parts.append(pass_on(b["part_out"].at[2], b["part_in"], "sq", "rq", 2, ahead))
    own = pl.ds(pl.multiple_of(t * share, share), share)
    output = attend(t)
    for k in range(8):
        other = flipped(place, k)
        shift = ((other[2] * 2 * s.nz + other[3]) * 2 + other[4]) * s.per
        b["hot_q"][k] = one_hot(first_rows(s), shift, local)
        b["hot_kv"][k] = one_hot(first_rows(s), shift - local, 2 * local)
    b_proj, merge_gain, merge_bias = (loaded(name) for name in ("b_proj", "merge_gain", "merge_bias"))
    output = output + vector(b_proj) + patches[own, :].astype(f32)
    upstream = b["up_out"][t].astype(f32)
    for i in (1, 2):
        ups[i].wait_recv()
        upstream = upstream + b["up_in"][i].astype(f32)
    for i in (1, 2):
        parts[i].wait_recv()
        output = output + b["part_in"][i].astype(f32)
    merged, unit_rows, inverse = normalize(output, vector(merge_gain), vector(merge_bias))
    b["row_out"][...] = normalize_back(upstream, unit_rows, inverse, vector(merge_gain)).astype(bf)
    half = share // 2

    def pass_rows(source, i, to):
        for c in range(2):
            piece = pl.ds(c * half, half)
            yield send_seq(
                source.at[piece], b["row_in"].at[i, piece], b["sr"].at[2 * i + c], b["rr"].at[2 * i + c], to
            )

    rows_sent = [[], [], []]
    for pieces in zip(pass_rows(b["row_out"], 0, ahead), pass_rows(b["row_out"], 1, behind)):
        for i in (0, 1):
            rows_sent[i].append(pieces[i])
    b["merged"][t] = merged.astype(bf)

    def joined(pieces, axis=0):
        return pieces[0] if len(pieces) == 1 else jnp.concatenate(pieces, axis=axis)

    def backward(row_grads, sources, first):
        places = [pl.ds(pl.multiple_of(source * share, share), share) for source in sources]
        attn = dims(joined(row_grads), w_proj[...], 1, 1).astype(bf)
        queries = joined([b["query"][rows, :] for rows in places])
        outs = []
        for h in range(heads):
            at = slice(h * HEAD, (h + 1) * HEAD)
            below = slice(local + h * HEAD, local + (h + 1) * HEAD)
            attn_h = attn[:, at]
            prob_grad = mm(attn_h, b["key_value"][below])
            probs = joined([b["probs"][h, rows, :] for rows in places])
            value_grad = dims(attn_h, probs.astype(bf), 0, 0)
            inner = jnp.sum(prob_grad * probs, axis=-1, keepdims=True)
            score_grad = (probs * (prob_grad - inner) * scaling).astype(bf)
            outs.append(dims(score_grad, b["key_value"][at], 1, 1))
            key_grad = dims(queries[:, at], score_grad, 0, 0)
            if first:
                b["kv_grad"][at] = key_grad
                b["kv_grad"][below] = value_grad
            else:
                b["kv_grad"][at] += key_grad
                b["kv_grad"][below] += value_grad
        value = jnp.concatenate(outs, axis=1).astype(bf)
        for i, rows in enumerate(places):
            b["query_grad"][rows, :] = value[i * share : (i + 1) * share]

    backward([b["row_out"][...]], [t], True)
    relayed = pass_rows(b["row_in"].at[0], 2, ahead)
    for copy in rows_sent[0]:
        copy.wait_recv()
        rows_sent[2].append(next(relayed))
    for copy in rows_sent[1]:
        copy.wait_recv()
    backward([b["row_in"][0], b["row_in"][1]], [behind, ahead], False)
    merged_sent = [
        send_seq(b["merged"].at[t], b["merged"].at[t], b["sm"].at[i], b["rm"].at[i], to)
        for i, to in enumerate((ahead, behind))
    ]
    for copy in rows_sent[2]:
        copy.wait_recv()
    backward([b["row_in"][2]], [across], False)

    kv_grad = b["kv_grad"][...].astype(bf)

    def permuted(k):
        value = dims(b["hot_q"][k], b["query_grad"][...], 1, 1) + mm(b["hot_kv"][k], kv_grad)
        return value.astype(bf)

    def relay():
        merged_sent[0].wait_recv()
        merged_sent.append(
            send_seq(b["merged"].at[behind], b["merged"].at[behind], b["sm"].at[2], b["rm"].at[2], ahead)
        )

    def between():
        for copy in merged_sent[1:]:
            copy.wait_recv()
        every = b["merged"][...].reshape(block, width)
        value = mm(select, every).astype(bf)
        for q in range(4):
            placed_ref[:, q * width : (q + 1) * width] = value[q * share : (q + 1) * share]

    clip_sum(s, place, permuted, shared, relay, between, summed_ref, b)
    for copies in (ups, parts, *rows_sent, merged_sent):
        for copy in copies:
            copy.wait_send()


def fused(s, n, **operands):
    block, width = operands["patches"].shape
    local = operands["w_proj"].shape[0]
    scratch = block_scratch(block, width, local, n) | reduce_scratch(s, width, block)
    for name in ORDER:
        space = pltpu.SMEM if name == "tokens" else pltpu.VMEM
        scratch["in_" + name] = space(operands[name].shape, operands[name].dtype)
    vmem = pl.BlockSpec(memory_space=pltpu.VMEM)
    return pl.pallas_call(
        functools.partial(block_kernel, s, n, tuple(scratch)),
        out_shape=(
            pltpu.VMEM((block // n, 4 * width), jnp.bfloat16),
            pltpu.VMEM((s.per, 1, width), jnp.float32),
        ),
        in_specs=[pl.BlockSpec(memory_space=pl.ANY)] * len(ORDER),
        out_specs=(vmem,) * 2,
        scratch_shapes=list(scratch.values()),
        compiler_params=pltpu.CompilerParams(
            collective_id=0, has_side_effects=True, vmem_limit_bytes=60000 * 1024
        ),
    )(*(operands[name] for name in ORDER))


def body(
    rows_y, rows_z, seq,
    patches, clip_tokens, positions, norm_gain, norm_bias, w_qkv, b_qkv, w_proj, b_proj,
    merge_gain, merge_bias, grad_placed,
):
    width = patches.shape[1]
    weights = w_qkv.transpose(1, 2, 0).reshape(-1, width)
    s = Sizes(rows_y, rows_z, width, weights.shape[0])
    placed, summed = fused(
        s, seq, tokens=clip_tokens, patches=patches, positions=positions, norm_gain=norm_gain,
        norm_bias=norm_bias, weights=weights, b_qkv=b_qkv, w_proj=w_proj, b_proj=b_proj,
        merge_gain=merge_gain, merge_bias=merge_bias, grads=grad_placed,
    )
    return placed, summed.transpose(1, 0, 2)


def build(mesh, rows_y, rows_z):
    placed = (
        P("clip", None), P("clip"), P("clip", None), P(), P(), P(None, None, "seq"),
        P(None, "seq"), P("seq", None), P(), P(), P(), P(("clip", "seq"), None),
    )
    return jax.shard_map(
        functools.partial(body, rows_y, rows_z, mesh.shape["seq"]),
        mesh=mesh,
        in_specs=placed,
        out_specs=(P(("clip", "seq"), None), P("seq", "clip", None)),
        check_vma=False,
    )


def solution(mesh):
    return build(mesh, 8, 12)
```

```python
import functools

import jax
import jax.numpy as jnp
import numpy as np
from jax import lax
from jax.experimental import pallas as pl
from jax.experimental.pallas import tpu as pltpu
from jax.sharding import PartitionSpec as P

HEAD = 80
MESH = pl.DeviceIdType.MESH
EPSILON = 1e-06


def one_hot(sources, shift, width):
    lanes = lax.broadcasted_iota(jnp.int32, (sources.shape[0], width), 1)
    return (lanes == sources + shift).astype(jnp.float32).astype(jnp.bfloat16)


def up_to(count, unit):
    return -(-count // unit) * unit


class Sizes:
    def __init__(self, rows_y, rows_z, width, rows):
        self.ny, self.nz = rows_y // 2, rows_z // 2
        self.rows = rows
        self.per = rows // (2 * rows_y * rows_z)
        self.ca = up_to(self.per * self.nz, 16)
        self.cb = up_to(self.per * self.ny, 8)
        self.wa = 6 * 128
        self.wb = width - self.wa
        self.ka, self.kb = self.wa // 128, self.wb // 128
        self.ra, self.rb = up_to(self.per * self.ka, 16), up_to(self.per * self.kb, 16)


def source_rows(groups, length, count, unit, steps):
    row = lax.broadcasted_iota(jnp.int32, (groups * length, 1), 0)
    group, inside = lax.div(row, length), lax.rem(row, length)
    major, minor = lax.div(inside, unit), lax.rem(inside, unit)
    source = group * steps[0] + major * steps[1] + minor
    return jnp.where(inside < count * unit, source, -100000)


def first_rows(s):
    return source_rows(s.ny, s.ca, s.nz, s.per, (8 * s.per * s.nz, 4 * s.per))


def second_rows(s):
    return source_rows(s.nz, s.cb, s.ny, s.per, (s.per, s.ca))


def third_rows(s):
    return source_rows(s.nz, s.ra, s.ka, s.per, (s.per, s.ca))


def fourth_rows(s):
    return source_rows(s.ny, s.rb, s.kb, s.per, (s.per, s.cb))


def tiles_down(values):
    return jnp.concatenate(
        [values[:, k : k + 128] for k in range(0, values.shape[1], 128)], axis=0
    )


def far_first(count):
    return sorted(range(1, count), key=lambda k: (-min(k, count - k), k))


def send(source, target, send_sem, recv_sem, clip):
    copy = pltpu.make_async_remote_copy(
        src_ref=source, dst_ref=target, send_sem=send_sem, recv_sem=recv_sem,
        device_id={"clip": clip}, device_id_type=MESH,
    )
    copy.start()
    return copy


def reduce_scratch(s, width, block):
    bf = jnp.bfloat16
    dma = pltpu.SemaphoreType.DMA
    return dict(
        hot_q=pltpu.VMEM((8, s.ny * s.ca, s.rows // 3), bf),
        hot_kv=pltpu.VMEM((8, s.ny * s.ca, s.rows // 3 * 2), bf),
        give=pltpu.VMEM((8, s.ny * s.ca, block), bf),
        got=pltpu.VMEM((8, s.ny * s.ca, block), bf),
        others=pltpu.VMEM((8, block, width), bf),
        out_a=pltpu.VMEM((s.ny, s.ca, s.wa), bf),
        in_a=pltpu.VMEM((s.ny, s.ca, s.wa), bf),
        out_b=pltpu.VMEM((s.nz, s.cb, s.wb), bf),
        in_b=pltpu.VMEM((s.nz, s.cb, s.wb), bf),
        out_c=pltpu.VMEM((s.nz, s.ra, 128), bf),
        in_c=pltpu.VMEM((s.nz, s.ra, 128), bf),
        out_d=pltpu.VMEM((s.ny, s.rb, 128), bf),
        in_d=pltpu.VMEM((s.ny, s.rb, 128), bf),
        sn=dma((8,)), rn=dma((8,)),
        sp=dma((8,)), rp=dma((8,)),
        sa=dma((s.ny,)), ra=dma((s.ny,)),
        sb=dma((s.nz,)), rb=dma((s.nz,)),
        sc=dma((s.nz,)), rc=dma((s.nz,)),
        sd=dma((s.ny,)), rd=dma((s.ny,)),
    )


def place_of(s):
    me = lax.axis_index("clip")
    core = lax.rem(me, 2)
    chip = lax.div(me, 2)
    z = lax.rem(chip, 2 * s.nz)
    y = lax.div(chip, 2 * s.nz)
    return lax.div(y, 2), lax.div(z, 2), lax.rem(y, 2), lax.rem(z, 2), core


def clip_of(s, place):
    y, z, odd_y, odd_z, core = place
    return ((2 * y + odd_y) * 2 * s.nz + 2 * z + odd_z) * 2 + core


def flipped(place, k):
    y, z, *bits = place
    return (y, z, *(1 - bit if k & (4 >> i) else bit for i, bit in enumerate(bits)))


def along_y(place, count, k):
    return (lax.rem(place[0] + k, count),) + place[1:]


def along_z(place, count, k):
    return (place[0], lax.rem(place[1] + k, count)) + place[2:]


def greet(s, place):
    barrier = pltpu.get_barrier_semaphore()
    others = [flipped(place, k) for k in range(1, 8)]
    others += [along_y(place, s.ny, k) for k in range(1, s.ny)]
    others += [along_z(place, s.nz, k) for k in range(1, s.nz)]
    for other in others:
        pl.semaphore_signal(
            barrier, inc=1, device_id={"clip": clip_of(s, other)}, device_id_type=MESH
        )
    return len(others)


def mm(left, right):
    return jnp.dot(left, right, preferred_element_type=jnp.float32)


def spread(s, out, arrived, send_sem, recv_sem, place, dim):
    along, count = ((along_y, s.ny), (along_z, s.nz))[dim]
    copies = []
    for k in far_first(count):
        other = along(place, count, k)
        copies.append((k, send(
            out.at[other[dim]], arrived.at[k], send_sem.at[k], recv_sem.at[k], clip_of(s, other)
        )))
    return copies


def added(out, arrived, copies, mine):
    total = out[mine].astype(jnp.float32)
    for k, copy in copies:
        copy.wait_recv()
        total = total + arrived[k].astype(jnp.float32)
    return total


def share_normed(s, place, b):
    copies = {}
    for k in (6, 4, 2, 1):
        copies[k] = send(
            b["normed"], b["others"].at[k], b["sn"].at[k], b["rn"].at[k], clip_of(s, flipped(place, k))
        )
    return copies


def clip_sum(s, place, permuted, normed, relay, between, summed_ref, b):
    y, z = place[:2]
    bf = jnp.bfloat16

    given = {}
    for k in (6, 7, 4, 5, 2, 3, 1):
        other = flipped(place, k)
        b["give"][k] = permuted(k)
        given[k] = send(b["give"].at[k], b["got"].at[k], b["sp"].at[k], b["rp"].at[k], clip_of(s, other))
    value = mm(permuted(0), b["normed"][...])
    relay()
    pair = clip_of(s, flipped(place, 1))
    for k in (2, 4, 6):
        normed[k].wait_recv()
        normed[k + 1] = send(
            b["others"].at[k], b["others"].at[k + 1], b["sn"].at[k + 1], b["rn"].at[k + 1], pair
        )
    for k in (1, 2, 4, 3, 5, 6, 7):
        if k & 1:
            normed[k].wait_recv()
        given[k].wait_recv()
        value = value + mm(b["got"][k], b["others"][k])
    b["out_a"][...] = value[:, : s.wa].reshape(s.ny, s.ca, s.wa).astype(bf)
    copies_a = spread(s, b["out_a"], b["in_a"], b["sa"], b["ra"], place, 0)
    value = mm(one_hot(second_rows(s), 0, s.ny * s.ca), value[:, s.wa :].astype(bf))
    b["out_b"][...] = value.reshape(s.nz, s.cb, s.wb).astype(bf)
    copies_b = spread(s, b["out_b"], b["in_b"], b["sb"], b["rb"], place, 1)
    between()
    total = tiles_down(added(b["out_a"], b["in_a"], copies_a, y)).astype(bf)
    value = mm(one_hot(third_rows(s), 0, s.ka * s.ca), total)
    b["out_c"][...] = value.reshape(s.nz, s.ra, 128).astype(bf)
    copies_c = spread(s, b["out_c"], b["in_c"], b["sc"], b["rc"], place, 1)
    total = tiles_down(added(b["out_b"], b["in_b"], copies_b, z)).astype(bf)
    value = mm(one_hot(fourth_rows(s), 0, s.kb * s.cb), total)
    b["out_d"][...] = value.reshape(s.ny, s.rb, 128).astype(bf)
    copies_d = spread(s, b["out_d"], b["in_d"], b["sd"], b["rd"], place, 0)
    total = added(b["out_c"], b["in_c"], copies_c, z)
    for k in range(s.ka):
        summed_ref[:, 0, k * 128 : (k + 1) * 128] = total[k * s.per : (k + 1) * s.per]
    total = added(b["out_d"], b["in_d"], copies_d, y)
    for k in range(s.kb):
        summed_ref[:, 0, s.wa + k * 128 : s.wa + (k + 1) * 128] = total[k * s.per : (k + 1) * s.per]
    for copies in (normed, given):
        for copy in copies.values():
            copy.wait_send()
    for copies in (copies_a, copies_b, copies_c, copies_d):
        for _, copy in copies:
            copy.wait_send()


def normalize(values, gain_row, bias_row):
    center = values - jnp.mean(values, axis=-1, keepdims=True)
    inverse = lax.rsqrt(jnp.mean(center * center, axis=-1, keepdims=True) + EPSILON)
    unit_rows = center * inverse
    return (unit_rows * gain_row + bias_row, unit_rows, inverse)


def normalize_back(upstream, unit_rows, inverse, gain_row):
    scaled = upstream * gain_row
    return inverse * (
        scaled
        - jnp.mean(scaled, axis=-1, keepdims=True)
        - unit_rows * jnp.mean(scaled * unit_rows, axis=-1, keepdims=True)
    )


def vector(ref):
    return ref[...].reshape(1, ref.shape[0])


def dims(left, right, a, b):
    return lax.dot_general(
        left, right, (((a,), (b,)), ((), ())), preferred_element_type=jnp.float32
    )


def send_seq(source, target, send_sem, recv_sem, seq):
    copy = pltpu.make_async_remote_copy(
        src_ref=source, dst_ref=target, send_sem=send_sem, recv_sem=recv_sem,
        device_id={"seq": seq}, device_id_type=MESH,
    )
    copy.start()
    return copy


def block_scratch(block, width, local, n):
    bf, f32 = jnp.bfloat16, jnp.float32
    dma = pltpu.SemaphoreType.DMA
    share = block // n
    return dict(
        normed=pltpu.VMEM((block, width), bf),
        query=pltpu.VMEM((block, local), bf),
        key_value=pltpu.VMEM((2 * local, block), bf),
        probs=pltpu.VMEM((local // HEAD, block, block), f32),
        biases=pltpu.VMEM((8, 384), f32),
        up_out=pltpu.VMEM((n, share, width), bf),
        up_in=pltpu.VMEM((3, share, width), bf),
        part_out=pltpu.VMEM((3, share, width), bf),
        part_in=pltpu.VMEM((3, share, width), bf),
        row_out=pltpu.VMEM((share, width), bf),
        row_in=pltpu.VMEM((3, share, width), bf),
        loads=dma((len(ORDER),)),
        merged=pltpu.VMEM((n, share, width), bf),
        query_grad=pltpu.VMEM((block, local), bf),
        kv_grad=pltpu.VMEM((2 * local, block), f32),
        su=dma((3,)), ru=dma((3,)),
        sq=dma((3,)), rq=dma((3,)),
        sr=dma((6,)), rr=dma((6,)),
        sm=dma((3,)), rm=dma((3,)),
    )


ORDER = (
    "tokens", "positions", "grads", "norm_gain", "norm_bias", "patches", "weights", "b_qkv",
    "w_proj", "b_proj", "merge_gain", "merge_bias",
)


def block_kernel(s, n, names, *refs):
    operands = tuple(zip(ORDER, refs[: len(ORDER)]))
    placed_ref, summed_ref, *scratch = refs[len(ORDER) :]
    b = dict(zip(names, scratch))
    loads = {}
    for i, (name, source) in enumerate(operands):
        loads[name] = pltpu.make_async_copy(source, b["in_" + name], b["loads"].at[i])
        loads[name].start()

    def loaded(name):
        loads[name].wait()
        return b["in_" + name]

    bf, f32, i32 = jnp.bfloat16, jnp.float32, jnp.int32
    patches, w_proj = b["in_patches"], b["in_w_proj"]
    block, width = patches.shape
    local = w_proj.shape[0]
    heads = local // HEAD
    share = block // n
    scaling = HEAD ** (-0.5)
    place = place_of(s)
    core = place[4]
    t = lax.axis_index("seq")
    ahead = lax.rem(t + 1 + 2 * core, n)
    behind = lax.rem(t + 3 - 2 * core, n)
    across = lax.rem(t + 2, n)
    partners = greet(s, place)
    for k in range(1, n):
        pl.semaphore_signal(
            pltpu.get_barrier_semaphore(), inc=1,
            device_id={"seq": lax.rem(t + k, n)}, device_id_type=MESH,
        )
    live = loaded("tokens")[0]

    spread_out = lax.broadcasted_iota(i32, (block // 4, block), 1)
    token_of = lax.broadcasted_iota(i32, (block // 4, block), 0)
    spread_out = ((spread_out >> 2) == token_of).astype(f32).astype(bf)
    places = jnp.broadcast_to(loaded("positions")[...].astype(f32), (8, block // 4)).astype(bf)
    places = mm(places, spread_out)[0:1].astype(i32)
    slot = lax.broadcasted_iota(i32, (1, block), 1)
    code = jnp.where(slot < 4 * live, places * 4 + (slot & 3), -1)
    row = lax.broadcasted_iota(i32, (4 * share, block), 0)
    wanted = (t * share + lax.rem(row, share)) * 4 + lax.div(row, share)
    select = (code == wanted).astype(f32).astype(bf)
    grads = loaded("grads")
    stacked = jnp.concatenate([grads[:, q * width : (q + 1) * width] for q in range(4)], axis=0)
    b["up_out"][...] = dims(select, stacked, 0, 0).reshape(n, share, width).astype(bf)
    pl.semaphore_wait(pltpu.get_barrier_semaphore(), partners + n - 1)
    def pass_on(out, arrived, sends, arrivals, i, to):
        return send_seq(out, arrived.at[i], b[sends].at[i], b[arrivals].at[i], to)

    ups = [
        pass_on(b["up_out"].at[across], b["up_in"], "su", "ru", 0, ahead),
        pass_on(b["up_out"].at[behind], b["up_in"], "su", "ru", 1, behind),
    ]
    norm_gain, norm_bias = loaded("norm_gain"), loaded("norm_bias")
    loaded("patches")
    b["normed"][...] = normalize(patches[...].astype(f32), vector(norm_gain), vector(norm_bias))[0].astype(bf)
    shared = share_normed(s, place, b)
    weights, b_qkv = loaded("weights"), loaded("b_qkv")
    normed = b["normed"][...]
    b["query"][...] = (dims(normed, weights[:local], 1, 1) + b_qkv[0:1]).astype(bf)
    b["biases"][...] = jnp.zeros((8, 384), f32)
    b["biases"][0:2, :local] = b_qkv[1:3]
    columns = b["biases"][...].T
    for p in (0, 1):
        value = dims(weights[(1 + p) * local : (2 + p) * local], normed, 1, 1)
        b["key_value"][p * local : (p + 1) * local] = (value + columns[:local, p : p + 1]).astype(bf)

    live_keys = lax.broadcasted_iota(i32, (share, block), 1) < 4 * live
    loaded("w_proj")
    parts = []

    def attend(to):
        rows = pl.ds(pl.multiple_of(to * share, share), share)
        queries = b["query"][rows, :]
        outs = []
        for h in range(heads):
            at = slice(h * HEAD, (h + 1) * HEAD)
            scores = mm(queries[:, at], b["key_value"][at]) * scaling
            scores = jnp.where(live_keys, scores, -1e30)
            powers = jnp.exp(scores - jnp.max(scores, axis=-1, keepdims=True))
            probs = powers * (1.0 / jnp.sum(powers, axis=-1, keepdims=True))
            b["probs"][h, rows, :] = probs
            outs.append(dims(probs.astype(bf), b["key_value"][local + h * HEAD : local + (h + 1) * HEAD], 1, 1))
        attended = jnp.concatenate(outs, axis=1).astype(bf)
        return mm(attended, w_proj[...])

    b["part_out"][0] = attend(across).astype(bf)
    parts.append(pass_on(b["part_out"].at[0], b["part_in"], "sq", "rq", 0, ahead))
    b["part_out"][1] = attend(behind).astype(bf)
    parts.append(pass_on(b["part_out"].at[1], b["part_in"], "sq", "rq", 1, behind))
    ups[0].wait_recv()
    b["up_out"][ahead] = (b["up_out"][ahead].astype(f32) + b["up_in"][0].astype(f32)).astype(bf)
    ups.append(pass_on(b["up_out"].at[ahead], b["up_in"], "su", "ru", 2, ahead))
    part = attend(ahead)
    parts[0].wait_recv()
    b["part_out"][2] = (part + b["part_in"][0].astype(f32)).astype(bf)
    parts.append(pass_on(b["part_out"].at[2], b["part_in"], "sq", "rq", 2, ahead))
    own = pl.ds(pl.multiple_of(t * share, share), share)
    output = attend(t)
    for k in range(8):
        other = flipped(place, k)
        shift = ((other[2] * 2 * s.nz + other[3]) * 2 + other[4]) * s.per
        b["hot_q"][k] = one_hot(first_rows(s), shift, local)
        b["hot_kv"][k] = one_hot(first_rows(s), shift - local, 2 * local)
    b_proj, merge_gain, merge_bias = (loaded(name) for name in ("b_proj", "merge_gain", "merge_bias"))
    output = output + vector(b_proj) + patches[own, :].astype(f32)
    upstream = b["up_out"][t].astype(f32)
    for i in (1, 2):
        ups[i].wait_recv()
        upstream = upstream + b["up_in"][i].astype(f32)
    for i in (1, 2):
        parts[i].wait_recv()
        output = output + b["part_in"][i].astype(f32)
    merged, unit_rows, inverse = normalize(output, vector(merge_gain), vector(merge_bias))
    b["row_out"][...] = normalize_back(upstream, unit_rows, inverse, vector(merge_gain)).astype(bf)
    half = share // 2

    def pass_rows(source, i, to):
        for c in range(2):
            piece = pl.ds(c * half, half)
            yield send_seq(
                source.at[piece], b["row_in"].at[i, piece], b["sr"].at[2 * i + c], b["rr"].at[2 * i + c], to
            )

    rows_sent = [[], [], []]
    for pieces in zip(pass_rows(b["row_out"], 0, ahead), pass_rows(b["row_out"], 1, behind)):
        for i in (0, 1):
            rows_sent[i].append(pieces[i])
    b["merged"][t] = merged.astype(bf)

    def joined(pieces, axis=0):
        return pieces[0] if len(pieces) == 1 else jnp.concatenate(pieces, axis=axis)

    def backward(row_grads, sources, first):
        places = [pl.ds(pl.multiple_of(source * share, share), share) for source in sources]
        attn = dims(joined(row_grads), w_proj[...], 1, 1).astype(bf)
        queries = joined([b["query"][rows, :] for rows in places])
        outs = []
        for h in range(heads):
            at = slice(h * HEAD, (h + 1) * HEAD)
            below = slice(local + h * HEAD, local + (h + 1) * HEAD)
            attn_h = attn[:, at]
            prob_grad = mm(attn_h, b["key_value"][below])
            probs = joined([b["probs"][h, rows, :] for rows in places])
            value_grad = dims(attn_h, probs.astype(bf), 0, 0)
            inner = jnp.sum(prob_grad * probs, axis=-1, keepdims=True)
            score_grad = (probs * (prob_grad - inner) * scaling).astype(bf)
            outs.append(dims(score_grad, b["key_value"][at], 1, 1))
            key_grad = dims(queries[:, at], score_grad, 0, 0)
            if first:
                b["kv_grad"][at] = key_grad
                b["kv_grad"][below] = value_grad
            else:
                b["kv_grad"][at] += key_grad
                b["kv_grad"][below] += value_grad
        value = jnp.concatenate(outs, axis=1).astype(bf)
        for i, rows in enumerate(places):
            b["query_grad"][rows, :] = value[i * share : (i + 1) * share]

    backward([b["row_out"][...]], [t], True)
    relayed = pass_rows(b["row_in"].at[0], 2, ahead)
    for copy in rows_sent[0]:
        copy.wait_recv()
        rows_sent[2].append(next(relayed))
    for copy in rows_sent[1]:
        copy.wait_recv()
    backward([b["row_in"][0], b["row_in"][1]], [behind, ahead], False)
    merged_sent = [
        send_seq(b["merged"].at[t], b["merged"].at[t], b["sm"].at[i], b["rm"].at[i], to)
        for i, to in enumerate((ahead, behind))
    ]
    for copy in rows_sent[2]:
        copy.wait_recv()
    backward([b["row_in"][2]], [across], False)

    kv_grad = b["kv_grad"][...].astype(bf)

    def permuted(k):
        value = dims(b["hot_q"][k], b["query_grad"][...], 1, 1) + mm(b["hot_kv"][k], kv_grad)
        return value.astype(bf)

    def relay():
        merged_sent[0].wait_recv()
        merged_sent.append(
            send_seq(b["merged"].at[behind], b["merged"].at[behind], b["sm"].at[2], b["rm"].at[2], ahead)
        )

    def between():
        for copy in merged_sent[1:]:
            copy.wait_recv()
        every = b["merged"][...].reshape(block, width)
        value = mm(select, every).astype(bf)
        for q in range(4):
            placed_ref[:, q * width : (q + 1) * width] = value[q * share : (q + 1) * share]

    clip_sum(s, place, permuted, shared, relay, between, summed_ref, b)
    for copies in (ups, parts, *rows_sent, merged_sent):
        for copy in copies:
            copy.wait_send()


def fused(s, n, **operands):
    block, width = operands["patches"].shape
    local = operands["w_proj"].shape[0]
    scratch = block_scratch(block, width, local, n) | reduce_scratch(s, width, block)
    for name in ORDER:
        space = pltpu.SMEM if name == "tokens" else pltpu.VMEM
        scratch["in_" + name] = space(operands[name].shape, operands[name].dtype)
    vmem = pl.BlockSpec(memory_space=pltpu.VMEM)
    return pl.pallas_call(
        functools.partial(block_kernel, s, n, tuple(scratch)),
        out_shape=(
            pltpu.VMEM((block // n, 4 * width), jnp.bfloat16),
            pltpu.VMEM((s.per, 1, width), jnp.float32),
        ),
        in_specs=[pl.BlockSpec(memory_space=pl.ANY)] * len(ORDER),
        out_specs=(vmem,) * 2,
        scratch_shapes=list(scratch.values()),
        compiler_params=pltpu.CompilerParams(
            collective_id=0, has_side_effects=True, vmem_limit_bytes=60000 * 1024
        ),
    )(*(operands[name] for name in ORDER))


def body(
    rows_y, rows_z, seq,
    patches, clip_tokens, positions, norm_gain, norm_bias, w_qkv, b_qkv, w_proj, b_proj,
    merge_gain, merge_bias, grad_placed,
):
    width = patches.shape[1]
    weights = w_qkv.transpose(1, 2, 0).reshape(-1, width)
    s = Sizes(rows_y, rows_z, width, weights.shape[0])
    placed, summed = fused(
        s, seq, tokens=clip_tokens, patches=patches, positions=positions, norm_gain=norm_gain,
        norm_bias=norm_bias, weights=weights, b_qkv=b_qkv, w_proj=w_proj, b_proj=b_proj,
        merge_gain=merge_gain, merge_bias=merge_bias, grads=grad_placed,
    )
    return placed, summed.transpose(1, 0, 2)


def build(mesh, rows_y, rows_z):
    placed = (
        P("clip", None), P("clip"), P("clip", None), P(), P(), P(None, None, "seq"),
        P(None, "seq"), P("seq", None), P(), P(), P(), P(("clip", "seq"), None),
    )
    return jax.shard_map(
        functools.partial(body, rows_y, rows_z, mesh.shape["seq"]),
        mesh=mesh,
        in_specs=placed,
        out_specs=(P(("clip", "seq"), None), P("seq", "clip", None)),
        check_vma=False,
    )


def solution(mesh):
    return build(mesh, 8, 12)
```
